64 devices in a mesh: dp: 4 (over x, y), wg: 16 (over z, core).
Axes of the slice: x: 2, y: 2, z: 8, core: 2. Of those that a mesh axis runs over, the one named last changes fastest.
The devices are a block of a 4x4x8 slice.
Arguments:
- x: bfloat16 [128, 128, 1024], P(('dp', 'wg')), parts along dimension 0
- positions: int32 [512], P('dp'), parts along dimension 0
- prompt_len: int32 [128], P(('dp', 'wg')), parts along dimension 0
- ln_attn: bfloat16 [2, 2, 1024], P(None, None, 'wg')
- ln_mlp: bfloat16 [2, 2, 1024], P(None, None, 'wg')
- w_qkv: bfloat16 [2, 1024, 3072], P(None, None, 'wg')
- w_out: bfloat16 [2, 16, 64, 1024], P(None, None, None, 'wg')
- w_up: bfloat16 [2, 1024, 4096], P(None, None, 'wg')
- w_down: bfloat16 [2, 4096, 1024], P(None, None, 'wg')
Outputs:
- output 1: bfloat16 [128, 128, 1024], P(('dp', 'wg')), parts along dimension 0
- output 2: bfloat16 [2, 128, 128, 16, 64], P(None, ('dp', 'wg')), parts along dimension 1
- output 3: bfloat16 [2, 128, 128, 16, 64], P(None, ('dp', 'wg')), parts along dimension 1
There are 4 independent parts. The reference program is written for one: setup_inputs(seed, part) draws one part's arguments, and reference() takes and returns one part's arrays. A program takes and returns all parts, laid end to end along the dimension named above; an argument that names none is the same for every part.
All inputs are finite; a program needn't handle non-finite values.
Results may differ from the reference program's by a relative error of at most 0.0119992.
Values are sent between devices in bfloat16 or wider.
A program may use at most 768 MiB of HBM per device.

```python
import jax
import jax.numpy as jnp
from jax import lax

D = 1024
HEADS = 16
KV_HEADS = 16
HEAD = 64
FF = 4096
LAYERS = 2
BATCH = 32
SEQ = 128

Q_PER = HEADS // KV_HEADS
QKV_COLS = KV_HEADS * (Q_PER + 2) * HEAD
EPSILON = 1e-5
ROPE_BASE = 10000.0


def norm_table(key_gain, key_bias):
    gain_rows = 1.0 + 0.25 * jax.random.normal(key_gain, (LAYERS, D), jnp.float32)
    bias_rows = 0.25 * jax.random.normal(key_bias, (LAYERS, D), jnp.float32)
    return jnp.stack([gain_rows, bias_rows], axis=1).astype(jnp.bfloat16)


def setup_inputs(seed: int = 0, part: int = 0) -> dict:
    root_key = jax.random.key(seed)
    part_key = jax.random.fold_in(root_key, part)
    key_x, key_pos, key_len = jax.random.split(part_key, 3)
    shared = jax.random.split(jax.random.key(seed + 1), 8)
    x = jax.random.normal(key_x, (BATCH, SEQ, D), jnp.float32).astype(jnp.bfloat16)
    pos_start = jax.random.randint(key_pos, (), 0, 2048, dtype=jnp.int32)
    positions = pos_start + jnp.arange(SEQ, dtype=jnp.int32)
    raw_lens = jax.random.randint(key_len, (BATCH,), max(1, SEQ // 4), SEQ + 1, dtype=jnp.int32)
    prompt_len = raw_lens.at[0].set(SEQ)
    col_gain = jnp.concatenate([jnp.full((Q_PER,), 2.0, jnp.float32), jnp.ones((2,), jnp.float32)])
    qkv_base = jax.random.normal(shared[4], (LAYERS, D, KV_HEADS, Q_PER + 2, HEAD), jnp.float32)
    w_qkv = (qkv_base * col_gain[:, None] * D ** -0.5).reshape(LAYERS, D, QKV_COLS).astype(jnp.bfloat16)
    w_out = (jax.random.normal(shared[5], (LAYERS, HEADS, HEAD, D), jnp.float32) * (2.0 * (HEADS * HEAD) ** -0.5)).astype(jnp.bfloat16)
    w_up = (jax.random.normal(shared[6], (LAYERS, D, FF), jnp.float32) * D ** -0.5).astype(jnp.bfloat16)
    w_down = (jax.random.normal(shared[7], (LAYERS, FF, D), jnp.float32) * FF ** -0.5).astype(jnp.bfloat16)
    return {'x': x, 'positions': positions, 'prompt_len': prompt_len, 'ln_attn': norm_table(shared[0], shared[1]), 'ln_mlp': norm_table(shared[2], shared[3]), 'w_qkv': w_qkv, 'w_out': w_out, 'w_up': w_up, 'w_down': w_down}


def layer_norm(tok_rows, norm_params):
    rows_f32 = tok_rows.astype(jnp.float32)
    row_mean = jnp.mean(rows_f32, axis=-1, keepdims=True)
    centered = rows_f32 - row_mean
    row_var = jnp.mean(centered * centered, axis=-1, keepdims=True)
    normed = centered * lax.rsqrt(row_var + EPSILON)
    return (normed * norm_params[0].astype(jnp.float32) + norm_params[1].astype(jnp.float32)).astype(jnp.bfloat16)


def rotary_tables(positions):
    half_dim = HEAD // 2
    inv_freq = ROPE_BASE ** (-jnp.arange(half_dim, dtype=jnp.float32) * 2.0 / HEAD)
    angles = positions.astype(jnp.float32)[:, None] * inv_freq[None, :]
    return jnp.cos(angles), jnp.sin(angles)


def apply_rotary(vec, cos_table, sin_table):
    half_dim = vec.shape[-1] // 2
    vec_f32 = vec.astype(jnp.float32)
    first_half = vec_f32[..., :half_dim]
    second_half = vec_f32[..., half_dim:]
    return jnp.concatenate([first_half * cos_table - second_half * sin_table, second_half * cos_table + first_half * sin_table], axis=-1).astype(jnp.bfloat16)


def prompt_layer(tok_rows, length, cos_table, sin_table, weights):
    ln_a, ln_m, w_qkv, w_out, w_up, w_down = weights
    h_attn = layer_norm(tok_rows, ln_a)
    h_mlp = layer_norm(tok_rows, ln_m)
    qkv_rows = jnp.dot(h_attn, w_qkv, preferred_element_type=jnp.float32).astype(jnp.bfloat16)
    grouped = qkv_rows.reshape(SEQ, KV_HEADS, Q_PER + 2, HEAD)
    query_rot = apply_rotary(grouped[:, :, :Q_PER, :], cos_table[:, None, None, :], sin_table[:, None, None, :])
    key_rot = apply_rotary(grouped[:, :, Q_PER, :], cos_table[:, None, :], sin_table[:, None, :])
    value_rows = grouped[:, :, Q_PER + 1, :]
    scores = jnp.einsum('qgph,kgh->gpqk', query_rot.astype(jnp.float32), key_rot.astype(jnp.float32)) * HEAD ** -0.5
    q_index = jnp.arange(SEQ)[:, None]
    k_index = jnp.arange(SEQ)[None, :]
    allowed = (k_index <= q_index) & (k_index < length)
    scores = jnp.where(allowed, scores, -1e30)
    prob_bf16 = jax.nn.softmax(scores, axis=-1).astype(jnp.bfloat16)
    context = jnp.einsum('gpqk,kgh->qgph', prob_bf16.astype(jnp.float32), value_rows.astype(jnp.float32)).astype(jnp.bfloat16)
    attn_out = jnp.dot(context.reshape(SEQ, HEADS * HEAD), w_out.reshape(HEADS * HEAD, D), preferred_element_type=jnp.float32)
    hidden = jax.nn.gelu(jnp.dot(h_mlp, w_up, preferred_element_type=jnp.float32), approximate=False).astype(jnp.bfloat16)
    mlp_out = jnp.dot(hidden, w_down, preferred_element_type=jnp.float32)
    new_rows = (tok_rows.astype(jnp.float32) + attn_out + mlp_out).astype(jnp.bfloat16)
    return new_rows, key_rot, value_rows


def reference(x, positions, prompt_len, ln_attn, ln_mlp, w_qkv, w_out, w_up, w_down):
    cos_table, sin_table = rotary_tables(positions)
    stacked = (ln_attn, ln_mlp, w_qkv, w_out, w_up, w_down)

    def one_prompt(prompt_item):
        tok_rows, length = prompt_item

        def layer_step(carry_rows, weights):
            new_rows, key_rot, value_rows = prompt_layer(carry_rows, length, cos_table, sin_table, weights)
            return new_rows, (key_rot, value_rows)

        final_rows, (key_layers, value_layers) = lax.scan(layer_step, tok_rows, stacked)
        return final_rows, key_layers, value_layers

    y, key_cache, value_cache = lax.map(one_prompt, (x, prompt_len))
    return y, jnp.swapaxes(key_cache, 0, 1), jnp.swapaxes(value_cache, 0, 1)
```

```python
import functools
import math

import jax
import jax.numpy as jnp
from jax import lax
from jax.experimental import pallas as pl
from jax.experimental.pallas import tpu as pltpu
from jax.sharding import PartitionSpec as P

EPSILON = 1e-5
ROPE_BASE = 10000.0
MESH = pl.DeviceIdType.MESH
F32 = jnp.float32
BF16 = jnp.bfloat16
QUARTERS = 4
UNITS = 3


def kernel(
    cols,
    chips,
    layers,
    x_hbm,
    cos_ref,
    sin_ref,
    len_ref,
    ln_ref,
    qkv_hbm,
    up_hbm,
    out_hbm,
    down_hbm,
    y_ref,
    k_ref,
    v_ref,
    buf_q,
    buf_u,
    buf_d,
    up_nat,
    out_nat,
    x_nat,
    x_t,
    a_t,
    m_t,
    ctx_t,
    hid_t,
    acc,
    ln_all,
    z_recv,
    xy_recv,
    sib_recv,
    z_send,
    xy_send,
    sib_send,
    ln_recv,
    ln_send,
    ln_sib,
    load_sem,
):
    half = chips // 2
    d_me = lax.axis_index("dp")
    w_me = lax.axis_index("wg")
    z, c = w_me // 2, w_me % 2
    x_pos, y_pos = d_me // cols, d_me % cols
    px, py = x_pos % 2, y_pos % 2
    dev_z = ({"wg": lax.rem(z + 1, chips) * 2 + c}, {"wg": lax.rem(z + chips - 1, chips) * 2 + c})
    dev_xy = ({"dp": d_me + cols * (1 - 2 * px)}, {"dp": d_me + 1 - 2 * py})
    dev_sib = {"wg": z * 2 + 1 - c}
    quarter_z = (px, 2 + py)
    quarter_xy = (1 - px, 3 - py)
    bufs = (buf_q, buf_u, buf_d)
    hops = ((half, half - 1), (half - 1, half))

    def chip_at(direction, h):
        return lax.rem(z + chips - h, chips) if direction == 0 else lax.rem(z + h, chips)

    def slot(chip, core, quarter):
        return (chip * 2 + core) * QUARTERS + quarter

    def remote(src, dst, send, recv, dev):
        return pltpu.make_async_remote_copy(
            src_ref=src, dst_ref=dst, send_sem=send, recv_sem=recv, device_id=dev, device_id_type=MESH
        )

    def z_copy(l, u, direction, s, h):
        ref = bufs[u].at[l, slot(chip_at(direction, h - 1), c, quarter_z[s])]
        return remote(ref, ref, z_send.at[l * UNITS + u, direction], z_recv.at[l * UNITS + u, direction * 2 + s, h - 1], dev_z[direction])

    def z_arrival(l, u, direction, s, h):
        ref = bufs[u].at[l, slot(chip_at(direction, h), c, quarter_z[s])]
        return remote(ref, ref, z_send.at[l * UNITS + u, direction], z_recv.at[l * UNITS + u, direction * 2 + s, h - 1], dev_z[direction])

    def source_index(direction, h):
        return (h - 1) * 2 + direction if h < half else chips - 2

    def xy_copy(l, u, direction, s, h, quarter):
        ref = bufs[u].at[l, slot(chip_at(direction, h), c, quarter)]
        return remote(ref, ref, xy_send.at[l * UNITS + u, s], xy_recv.at[l * UNITS + u, s, source_index(direction, h)], dev_xy[s])

    def sib_copy(l, u, chip, core, index):
        ref = bufs[u].at[l, pl.ds(slot(chip, core, 0), QUARTERS)]
        return remote(ref, ref, sib_send.at[l * UNITS + u], sib_recv.at[l * UNITS + u, index], dev_sib)

    def send_own(l, u, s):
        for direction in (0, 1):
            z_copy(l, u, direction, s, 1).start()

    def send_own_sib(l, u):
        sib_copy(l, u, z, c, chips - 1).start()

    def forward(l, u, h, s):
        for direction in (0, 1):
            if h > hops[direction][s]:
                continue
            z_arrival(l, u, direction, s, h).wait_recv()
            if h < hops[direction][s]:
                z_copy(l, u, direction, s, h + 1).start()
            xy_copy(l, u, direction, s, h, quarter_z[s]).start()

    def sources(h):
        return (0, 1) if h < half else (0,)

    def share_with_sibling(l, u, h):
        for direction in sources(h):
            for s in (0, 1):
                xy_copy(l, u, direction, s, h, quarter_xy[s]).wait_recv()
            sib_copy(l, u, chip_at(direction, h), c, source_index(direction, h)).start()

    def wait_sibling(l, u, h):
        for direction in sources(h):
            sib_copy(l, u, chip_at(direction, h), 1 - c, source_index(direction, h)).wait_recv()
        if h == half:
            sib_copy(l, u, z, 1 - c, chips - 1).wait_recv()

    def ln_hop(h):
        for direction in (0, 1):
            limit = half - direction
            if h > limit:
                continue
            if h > 0:
                ref = ln_all.at[c, chip_at(direction, h)]
                remote(ref, ref, ln_send.at[direction], ln_recv.at[direction, h - 1], dev_z[direction]).wait_recv()
            if h < limit:
                dst = ln_all.at[c, chip_at(direction, h)]
                src = ln_ref if h == 0 else dst
                remote(src, dst, ln_send.at[direction], ln_recv.at[direction, h], dev_z[direction]).start()

    def ln_share(core):
        return remote(ln_all.at[core], ln_all.at[core], ln_sib.at[0], ln_sib.at[1], dev_sib)


    def normalize(l):
        rows = x_t[...].reshape(-1, x_t.shape[-1]).astype(F32)
        centered = rows - jnp.mean(rows, axis=0, keepdims=True)
        var = jnp.mean(centered * centered, axis=0, keepdims=True)
        normed = centered * lax.rsqrt(var + EPSILON)
        params = ln_all[:, :, l].reshape(-1, 128).T
        step = x_t.shape[1]
        for w in range(2 * chips):
            block = normed[w * step : (w + 1) * step]
            base = ((w % 2) * chips + w // 2) * 8
            column = [params[:step, base + r : base + r + 1] for r in range(4)]
            a_t[w * step : (w + 1) * step, :] = (block * column[0] + column[1]).astype(BF16)
            m_t[w * step : (w + 1) * step, :] = (block * column[2] + column[3]).astype(BF16)

    def rotate(vec, cos, sin):
        first, second = vec[: cos.shape[0]].astype(F32), vec[cos.shape[0] :].astype(F32)
        return jnp.concatenate([first * cos - second * sin, second * cos + first * sin], axis=0).astype(BF16)

    def compute_qkv(l, chip):
        head_dim = k_ref.shape[3]
        seq = k_ref.shape[4]
        cos, sin = cos_ref[...], sin_ref[...]
        k_index = lax.broadcasted_iota(jnp.int32, (seq, seq), 0)
        q_index = lax.broadcasted_iota(jnp.int32, (seq, seq), 1)
        for core in (0, 1):
            head = chip * 2 + core
            share = buf_q[l, pl.ds(slot(chip, core, 0), QUARTERS)]
            share = share.reshape(-1, share.shape[-1])
            qkv = jnp.dot(share, a_t[...], preferred_element_type=F32).astype(BF16)
            for b in range(k_ref.shape[1]):
                cols_b = slice(b * seq, (b + 1) * seq)
                q_t = rotate(qkv[:head_dim, cols_b], cos, sin)
                k_t = rotate(qkv[head_dim : 2 * head_dim, cols_b], cos, sin)
                v_t = qkv[2 * head_dim :, cols_b]
                k_ref[l, b, head] = k_t
                v_ref[l, b, head] = v_t
                scores = jnp.dot(k_t.T, q_t, preferred_element_type=F32) * head_dim**-0.5
                allowed = (k_index <= q_index) & (k_index < len_ref[b])
                scores = jnp.where(allowed, scores, -1e30)
                top = jnp.max(scores, axis=0, keepdims=True)
                expo = jnp.exp(scores - top)
                prob = (expo * (1.0 / jnp.sum(expo, axis=0, keepdims=True))).astype(BF16)
                ctx_t[head, :, cols_b] = jnp.dot(v_t, prob, preferred_element_type=F32).astype(BF16)

    def compute_up(l, chip):
        up_rows = up_hbm.shape[2] // QUARTERS
        for core in (0, 1):
            share = buf_u[l, pl.ds(slot(chip, core, 0), QUARTERS), :up_rows, :]
            share = share.reshape(-1, share.shape[-1])
            pre = jnp.dot(share, m_t[...], preferred_element_type=F32)
            hid_t[chip * 2 + core] = (0.5 * pre * (1.0 + lax.erf(pre * 0.5**0.5))).astype(BF16)
        share = buf_u[l, pl.ds(slot(chip, 0, 0), 2 * QUARTERS), up_rows:, :]
        share = share.reshape(-1, share.shape[-1])
        ctx = ctx_t[...].reshape(-1, ctx_t.shape[-1])
        attn_out = jnp.dot(share, ctx, preferred_element_type=F32)
        acc[pl.ds(chip * 2, 2)] = attn_out.reshape((2,) + acc.shape[1:])

    def compute_down(l, chip):
        share = buf_d[l, pl.ds(slot(chip, 0, 0), 2 * QUARTERS)]
        share = share.reshape(-1, share.shape[-1])
        hidden = hid_t[...].reshape(-1, hid_t.shape[-1])
        mlp_out = jnp.dot(share, hidden, preferred_element_type=F32).reshape((2,) + acc.shape[1:])
        both = pl.ds(chip * 2, 2)
        x_t[both] = (x_t[both].astype(F32) + acc[both] + mlp_out).astype(BF16)

    computes = (compute_qkv, compute_up, compute_down)

    def compute(l, u, h):
        wait_sibling(l, u, h)
        if u == 0 and h == 1:

            @pl.when(l == 0)
            def _():
                ln_share(1 - c).wait_recv()

            normalize(l)

        @pl.loop(0, 2)
        def _(i):
            shift = chips - h + i * 2 * h if h < half else half + i * half
            computes[u](l, lax.rem(z + shift, chips))


    own = pl.ds(slot(z, c, 0), QUARTERS)
    loads = [pltpu.make_async_copy(qkv_hbm.at[l], buf_q.at[l, own], load_sem.at[l]) for l in range(layers)]
    loads += [pltpu.make_async_copy(down_hbm.at[l], buf_d.at[l, own], load_sem.at[layers + l]) for l in range(layers)]
    load_up = pltpu.make_async_copy(up_hbm, up_nat, load_sem.at[2 * layers])
    load_out = pltpu.make_async_copy(out_hbm, out_nat, load_sem.at[2 * layers + 1])
    load_x = pltpu.make_async_copy(x_hbm, x_nat, load_sem.at[2 * layers + 2])
    loads[0].start()
    load_x.start()
    load_up.start()
    load_out.start()
    for load in loads[1:]:
        load.start()

    barrier = pltpu.get_barrier_semaphore()
    neighbours = dev_z + dev_xy + (dev_sib,)
    for dev in neighbours:
        pl.semaphore_signal(barrier, inc=1, device_id=dev, device_id_type=MESH)
    ln_all[c, z] = ln_ref[...]
    loads[0].wait()
    pl.semaphore_wait(barrier, len(neighbours))

    ln_hop(0)
    send_own(0, 0, 0)
    send_own(0, 0, 1)
    send_own_sib(0, 0)
    load_x.wait()
    seq = x_hbm.shape[1]
    for b in range(x_hbm.shape[0]):
        x_t[:, :, b * seq : (b + 1) * seq] = x_nat[b].T.reshape(x_t.shape[0], x_t.shape[1], seq)
    ln_hop(1)
    load_up.wait()
    load_out.wait()
    up_rows = up_hbm.shape[2] // QUARTERS

    def place_up(l):
        up_t = up_nat[l].T
        buf_u[l, own, :up_rows, :] = up_t.reshape(QUARTERS, up_rows, up_t.shape[-1])
        out_t = out_nat[l].T
        buf_u[l, own, up_rows:, :] = out_t.reshape(QUARTERS, -1, out_t.shape[-1])

    place_up(0)


    order = [(u, h) for u in range(UNITS) for h in range(1, half + 1)]

    def back(n, k):
        return (order[n - k], 0) if n >= k else (order[n - k], -1)

    @pl.loop(0, layers)
    def _(l):
        first = l == 0

        def lagged(action, n, k):
            (u, h), offset = back(n, k)
            if offset == 0:
                action(l, u, h)
            else:

                @pl.when(l > 0)
                def _():
                    action(l - 1, u, h)

        for n, (u, h) in enumerate(order):
            if u == 0 and h <= 2:

                @pl.when(first)
                def _():
                    ln_hop(2 * h)

            forward(l, u, h, 0)
            if u == 0 and h == 1:

                @pl.when(first)
                def _():
                    ln_hop(3)

            forward(l, u, h, 1)
            if u == 0 and h == 2:

                @pl.when(first)
                def _():
                    ln_share(c).start()
                    for load in loads[1:]:
                        load.wait()
                    place_up(1)

            if h == half - 1:
                if u + 1 < UNITS:
                    for s in (0, 1):
                        send_own(l, u + 1, s)
                    send_own_sib(l, u + 1)
                else:

                    @pl.when(l + 1 < layers)
                    def _():
                        for s in (0, 1):
                            send_own(l + 1, 0, s)
                        send_own_sib(l + 1, 0)

            lagged(share_with_sibling, n, 1)
            lagged(compute, n, 2)

    last = layers - 1
    share_with_sibling(last, UNITS - 1, half)
    compute(last, UNITS - 1, half - 1)
    compute(last, UNITS - 1, half)
    y_t = x_t[...].reshape(-1, x_t.shape[-1])
    for b in range(y_ref.shape[0]):
        y_ref[b] = y_t[:, b * seq : (b + 1) * seq].T

    ref = ln_all.at[c]
    for direction in (0, 1):
        src = ref.at[pl.ds(0, half - direction)]
        remote(src, src, ln_send.at[direction], ln_sib.at[1], dev_z[direction]).wait_send()
    ln_share(c).wait_send()

    @pl.loop(0, layers)
    def _(l):
        for u in range(UNITS):
            sent = bufs[u].at[l, pl.ds(0, chips - 1)]
            for i in (0, 1):
                remote(sent, sent, z_send.at[l * UNITS + u, i], ln_sib.at[1], dev_z[i]).wait_send()
                remote(sent, sent, xy_send.at[l * UNITS + u, i], ln_sib.at[1], dev_xy[i]).wait_send()
            sent = bufs[u].at[l, pl.ds(0, chips * QUARTERS)]
            remote(sent, sent, sib_send.at[l * UNITS + u], ln_sib.at[1], dev_sib).wait_send()


def solution(mesh):
    batch_spec = P(("dp", "wg"))
    col_spec = P(None, None, "wg")
    out_spec = P(None, None, None, "wg")
    cache_spec = P(None, ("dp", "wg"))
    cols = math.isqrt(mesh.shape["dp"])
    chips = mesh.shape["wg"] // 2

    def local_program(x, positions, prompt_len, ln_attn, ln_mlp, w_qkv, w_out, w_up, w_down):
        prompts, seq, width = x.shape
        layers = w_qkv.shape[0]
        heads, head_dim = w_out.shape[1], w_out.shape[2]
        tokens = prompts * seq
        inv_freq = ROPE_BASE ** (-jnp.arange(head_dim // 2, dtype=F32) * 2.0 / head_dim)
        angles = inv_freq[:, None] * positions.astype(F32)[None, :]
        ln_rows = jnp.concatenate([ln_attn, ln_mlp], axis=1).astype(F32)
        ln_rows = jnp.pad(ln_rows, ((0, 0), (0, 8 - ln_rows.shape[1]), (0, 128 - ln_rows.shape[2])))
        qkv_t = jnp.swapaxes(w_qkv, 1, 2).reshape(layers, QUARTERS, -1, width)
        down_t = jnp.swapaxes(w_down, 1, 2).reshape(layers, QUARTERS, -1, w_down.shape[1])
        out_nat = w_out.reshape(layers, heads * head_dim, -1)
        up_rows = w_up.shape[2] // QUARTERS
        out_rows = out_nat.shape[2] // QUARTERS
        slots = chips * 2 * QUARTERS
        any_spec = pl.BlockSpec(memory_space=pl.ANY)
        vmem_spec = pl.BlockSpec(memory_space=pltpu.VMEM)
        cache = jax.ShapeDtypeStruct((layers, prompts, heads, head_dim, seq), BF16)
        dma = pltpu.SemaphoreType.DMA
        shares = chips * 2
        y, k_cache, v_cache = pl.pallas_call(
            functools.partial(kernel, cols, chips, layers),
            out_shape=(jax.ShapeDtypeStruct(x.shape, BF16), cache, cache),
            in_specs=[
                any_spec,
                vmem_spec,
                vmem_spec,
                pl.BlockSpec(memory_space=pltpu.SMEM),
                vmem_spec,
                any_spec,
                any_spec,
                any_spec,
                any_spec,
            ],
            out_specs=(vmem_spec, vmem_spec, vmem_spec),
            scratch_shapes=[
                pltpu.VMEM((layers, slots) + qkv_t.shape[2:], BF16),
                pltpu.VMEM((layers, slots, up_rows + out_rows, width), BF16),
                pltpu.VMEM((layers, slots) + down_t.shape[2:], BF16),
                pltpu.VMEM(w_up.shape, BF16),
                pltpu.VMEM(out_nat.shape, BF16),
                pltpu.VMEM(x.shape, BF16),
                pltpu.VMEM((shares, width // shares, tokens), BF16),
                pltpu.VMEM((width, tokens), BF16),
                pltpu.VMEM((width, tokens), BF16),
                pltpu.VMEM((heads, head_dim, tokens), BF16),
                pltpu.VMEM((shares, w_up.shape[2], tokens), BF16),
                pltpu.VMEM((shares, width // shares, tokens), F32),
                pltpu.VMEM((2, chips) + ln_rows.shape, F32),
                dma((layers * UNITS, 4, chips // 2)),
                dma((layers * UNITS, 2, chips - 1)),
                dma((layers * UNITS, chips)),
                dma((layers * UNITS, 2)),
                dma((layers * UNITS, 2)),
                dma((layers * UNITS,)),
                dma((2, chips // 2)),
                dma((2,)),
                dma((2,)),
                dma((2 * layers + 3,)),
            ],
            compiler_params=pltpu.CompilerParams(
                collective_id=0, has_side_effects=True, vmem_limit_bytes=67043328
            ),
        )(x, jnp.cos(angles), jnp.sin(angles), prompt_len, ln_rows, qkv_t, w_up, out_nat, down_t)
        order = (0, 1, 4, 2, 3)
        return y, k_cache.transpose(order), v_cache.transpose(order)

    return jax.shard_map(
        local_program,
        mesh=mesh,
        in_specs=(batch_spec, P("dp"), batch_spec, col_spec, col_spec, col_spec, out_spec, col_spec, col_spec),
        out_specs=(batch_spec, cache_spec, cache_spec),
        check_vma=False,
    )
```

```python
import functools
import math

import jax
import jax.numpy as jnp
from jax import lax
from jax.experimental import pallas as pl
from jax.experimental.pallas import tpu as pltpu
from jax.sharding import PartitionSpec as P

EPSILON = 1e-5
ROPE_BASE = 10000.0
MESH = pl.DeviceIdType.MESH
F32 = jnp.float32
BF16 = jnp.bfloat16
QUARTERS = 4
UNITS = 3


def kernel(
    cols,
    chips,
    layers,
    pos_ref,
    len_ref,
    x_hbm,
    lna_hbm,
    lnm_hbm,
    qkv_hbm,
    up_hbm,
    out_hbm,
    down_hbm,
    y_hbm,
    k_hbm,
    v_hbm,
    buf_q,
    buf_u,
    buf_d,
    up_nat,
    out_nat,
    x_nat,
    x_t,
    a_t,
    m_t,
    ctx_t,
    hid_t,
    acc,
    ln_all,
    ln_own,
    ln_nat,
    cos_ref,
    sin_ref,
    k_ref,
    v_ref,
    z_recv,
    xy_recv,
    sib_recv,
    z_send,
    xy_send,
    sib_send,
    ln_recv,
    ln_send,
    ln_sib,
    load_sem,
    cache_sem,
):
    half = chips // 2
    d_me = lax.axis_index("dp")
    w_me = lax.axis_index("wg")
    z, c = w_me // 2, w_me % 2
    x_pos, y_pos = d_me // cols, d_me % cols
    px, py = x_pos % 2, y_pos % 2
    dev_z = ({"wg": lax.rem(z + 1, chips) * 2 + c}, {"wg": lax.rem(z + chips - 1, chips) * 2 + c})
    dev_xy = ({"dp": d_me + cols * (1 - 2 * px)}, {"dp": d_me + 1 - 2 * py})
    dev_sib = {"wg": z * 2 + 1 - c}
    quarter_z = (px, 2 + py)
    quarter_xy = (1 - px, 3 - py)
    bufs = (buf_q, buf_u, buf_d)
    hops = ((half, half - 1), (half - 1, half))

    def chip_at(direction, h):
        return lax.rem(z + chips - h, chips) if direction == 0 else lax.rem(z + h, chips)

    def slot(chip, core, quarter):
        return (chip * 2 + core) * QUARTERS + quarter

    def remote(src, dst, send, recv, dev):
        return pltpu.make_async_remote_copy(
            src_ref=src, dst_ref=dst, send_sem=send, recv_sem=recv, device_id=dev, device_id_type=MESH
        )

    def z_copy(l, u, direction, s, h):
        ref = bufs[u].at[l, slot(chip_at(direction, h - 1), c, quarter_z[s])]
        return remote(ref, ref, z_send.at[l * UNITS + u, direction], z_recv.at[l * UNITS + u, direction * 2 + s, h - 1], dev_z[direction])

    def z_arrival(l, u, direction, s, h):
        ref = bufs[u].at[l, slot(chip_at(direction, h), c, quarter_z[s])]
        return remote(ref, ref, z_send.at[l * UNITS + u, direction], z_recv.at[l * UNITS + u, direction * 2 + s, h - 1], dev_z[direction])

    def source_index(direction, h):
        return (h - 1) * 2 + direction if h < half else chips - 2

    def xy_copy(l, u, direction, s, h, quarter):
        ref = bufs[u].at[l, slot(chip_at(direction, h), c, quarter)]
        return remote(ref, ref, xy_send.at[l * UNITS + u, s], xy_recv.at[l * UNITS + u, s, source_index(direction, h)], dev_xy[s])

    def sib_copy(l, u, chip, core, index):
        ref = bufs[u].at[l, pl.ds(slot(chip, core, 0), QUARTERS)]
        return remote(ref, ref, sib_send.at[l * UNITS + u], sib_recv.at[l * UNITS + u, index], dev_sib)

    def send_own(l, u, s):
        for direction in (0, 1):
            z_copy(l, u, direction, s, 1).start()

    def send_own_sib(l, u):
        sib_copy(l, u, z, c, chips - 1).start()

    def forward(l, u, h, s):
        for direction in (0, 1):
            if h > hops[direction][s]:
                continue
            z_arrival(l, u, direction, s, h).wait_recv()
            if h < hops[direction][s]:
                z_copy(l, u, direction, s, h + 1).start()
            xy_copy(l, u, direction, s, h, quarter_z[s]).start()

    def sources(h):
        return (0, 1) if h < half else (0,)

    def share_with_sibling(l, u, h):
        for direction in sources(h):
            for s in (0, 1):
                xy_copy(l, u, direction, s, h, quarter_xy[s]).wait_recv()
            sib_copy(l, u, chip_at(direction, h), c, source_index(direction, h)).start()

    def wait_sibling(l, u, h):
        for direction in sources(h):
            sib_copy(l, u, chip_at(direction, h), 1 - c, source_index(direction, h)).wait_recv()
        if h == half:
            sib_copy(l, u, z, 1 - c, chips - 1).wait_recv()

    def ln_hop(h):
        for direction in (0, 1):
            limit = half - direction
            if h > limit:
                continue
            if h > 0:
                ref = ln_all.at[c, chip_at(direction, h)]
                remote(ref, ref, ln_send.at[direction], ln_recv.at[direction, h - 1], dev_z[direction]).wait_recv()
            if h < limit:
                dst = ln_all.at[c, chip_at(direction, h)]
                src = ln_own if h == 0 else dst
                remote(src, dst, ln_send.at[direction], ln_recv.at[direction, h], dev_z[direction]).start()

    def ln_share(core):
        return remote(ln_all.at[core], ln_all.at[core], ln_sib.at[0], ln_sib.at[1], dev_sib)


    def normalize(l):
        rows = x_t[...].reshape(-1, x_t.shape[-1]).astype(F32)
        centered = rows - jnp.mean(rows, axis=0, keepdims=True)
        var = jnp.mean(centered * centered, axis=0, keepdims=True)
        normed = centered * lax.rsqrt(var + EPSILON)
        params = ln_all[:, :, l].reshape(-1, 128).T
        step = x_t.shape[1]
        for w in range(2 * chips):
            block = normed[w * step : (w + 1) * step]
            base = ((w % 2) * chips + w // 2) * 8
            column = [params[:step, base + r : base + r + 1] for r in range(4)]
            a_t[w * step : (w + 1) * step, :] = (block * column[0] + column[1]).astype(BF16)
            m_t[w * step : (w + 1) * step, :] = (block * column[2] + column[3]).astype(BF16)

    def rotate(vec, cos, sin):
        first, second = vec[: cos.shape[0]].astype(F32), vec[cos.shape[0] :].astype(F32)
        return jnp.concatenate([first * cos - second * sin, second * cos + first * sin], axis=0).astype(BF16)

    def compute_qkv(l, chip):
        head_dim = k_ref.shape[3]
        seq = k_ref.shape[4]
        cos, sin = cos_ref[...], sin_ref[...]
        k_index = lax.broadcasted_iota(jnp.int32, (seq, seq), 0)
        q_index = lax.broadcasted_iota(jnp.int32, (seq, seq), 1)
        for core in (0, 1):
            head = chip * 2 + core
            share = buf_q[l, pl.ds(slot(chip, core, 0), QUARTERS)]
            share = share.reshape(-1, share.shape[-1])
            qkv = jnp.dot(share, a_t[...], preferred_element_type=F32).astype(BF16)
            for b in range(k_ref.shape[1]):
                cols_b = slice(b * seq, (b + 1) * seq)
                q_t = rotate(qkv[:head_dim, cols_b], cos, sin)
                k_t = rotate(qkv[head_dim : 2 * head_dim, cols_b], cos, sin)
                v_t = qkv[2 * head_dim :, cols_b]
                k_ref[l, b, head] = k_t
                v_ref[l, b, head] = v_t
                scores = jnp.dot(k_t.T, q_t, preferred_element_type=F32) * head_dim**-0.5
                allowed = (k_index <= q_index) & (k_index < len_ref[b])
                scores = jnp.where(allowed, scores, -1e30)
                top = jnp.max(scores, axis=0, keepdims=True)
                expo = jnp.exp(scores - top)
                prob = (expo * (1.0 / jnp.sum(expo, axis=0, keepdims=True))).astype(BF16)
                ctx_t[head, :, cols_b] = jnp.dot(v_t, prob, preferred_element_type=F32).astype(BF16)

    def compute_up(l, chip):
        up_rows = up_hbm.shape[2] // QUARTERS
        for core in (0, 1):
            share = buf_u[l, pl.ds(slot(chip, core, 0), QUARTERS), :up_rows, :]
            share = share.reshape(-1, share.shape[-1])
            pre = jnp.dot(share, m_t[...], preferred_element_type=F32)
            hid_t[chip * 2 + core] = (0.5 * pre * (1.0 + lax.erf(pre * 0.5**0.5))).astype(BF16)
        share = buf_u[l, pl.ds(slot(chip, 0, 0), 2 * QUARTERS), up_rows:, :]
        share = share.reshape(-1, share.shape[-1])
        ctx = ctx_t[...].reshape(-1, ctx_t.shape[-1])
        attn_out = jnp.dot(share, ctx, preferred_element_type=F32)
        acc[pl.ds(chip * 2, 2)] = attn_out.reshape((2,) + acc.shape[1:])

    def compute_down(l, chip):
        share = buf_d[l, pl.ds(slot(chip, 0, 0), 2 * QUARTERS)]
        share = share.reshape(-1, share.shape[-1])
        hidden = hid_t[...].reshape(-1, hid_t.shape[-1])
        mlp_out = jnp.dot(share, hidden, preferred_element_type=F32).reshape((2,) + acc.shape[1:])
        both = pl.ds(chip * 2, 2)
        x_t[both] = (x_t[both].astype(F32) + acc[both] + mlp_out).astype(BF16)

    computes = (compute_qkv, compute_up, compute_down)

    def compute(l, u, h):
        wait_sibling(l, u, h)
        if u == 0 and h == 1:

            @pl.when(l == 0)
            def _():
                ln_share(1 - c).wait_recv()

            normalize(l)

        @pl.loop(0, 2)
        def _(i):
            shift = chips - h + i * 2 * h if h < half else half + i * half
            computes[u](l, lax.rem(z + shift, chips))


    own = pl.ds(slot(z, c, 0), QUARTERS)
    loads = [pltpu.make_async_copy(qkv_hbm.at[l], buf_q.at[l, own], load_sem.at[l]) for l in range(layers)]
    loads += [pltpu.make_async_copy(down_hbm.at[l], buf_d.at[l, own], load_sem.at[layers + l]) for l in range(layers)]
    load_up = pltpu.make_async_copy(up_hbm, up_nat, load_sem.at[2 * layers])
    load_out = pltpu.make_async_copy(out_hbm, out_nat, load_sem.at[2 * layers + 1])
    load_x = pltpu.make_async_copy(x_hbm, x_nat, load_sem.at[2 * layers + 2])
    load_ln = [pltpu.make_async_copy(src, ln_nat.at[i], load_sem.at[2 * layers + 3 + i]) for i, src in enumerate((lna_hbm, lnm_hbm))]
    for load in [loads[0]] + load_ln + [load_x, load_up, load_out] + loads[1:]:
        load.start()

    barrier = pltpu.get_barrier_semaphore()
    neighbours = dev_z + dev_xy + (dev_sib,)
    for dev in neighbours:
        pl.semaphore_signal(barrier, inc=1, device_id=dev, device_id_type=MESH)
    ln_own[...] = jnp.zeros_like(ln_own)
    for i in (0, 1):
        load_ln[i].wait()
        for l in range(layers):
            ln_own[l, 2 * i : 2 * i + 2, : ln_nat.shape[3]] = ln_nat[i, l].astype(F32)
    ln_all[c, z] = ln_own[...]
    loads[0].wait()
    pl.semaphore_wait(barrier, len(neighbours))

    send_own(0, 0, 0)
    send_own(0, 0, 1)
    ln_hop(0)
    send_own_sib(0, 0)
    load_x.wait()
    seq = x_hbm.shape[1]
    for b in range(x_hbm.shape[0]):
        x_t[:, :, b * seq : (b + 1) * seq] = x_nat[b].T.reshape(x_t.shape[0], x_t.shape[1], seq)
    half_dim = cos_ref.shape[0]
    row = lax.broadcasted_iota(jnp.int32, cos_ref.shape, 0).astype(F32)
    position = (pos_ref[0] + lax.broadcasted_iota(jnp.int32, cos_ref.shape, 1)).astype(F32)
    angles = position * ROPE_BASE ** (-row * 2.0 / (2 * half_dim))
    cos_ref[...] = jnp.cos(angles)
    sin_ref[...] = jnp.sin(angles)
    load_up.wait()
    load_out.wait()
    up_rows = up_hbm.shape[2] // QUARTERS

    def place_up(l):
        up_t = up_nat[l].T
        buf_u[l, own, :up_rows, :] = up_t.reshape(QUARTERS, up_rows, up_t.shape[-1])
        out_t = out_nat[l].T
        buf_u[l, own, up_rows:, :] = out_t.reshape(QUARTERS, -1, out_t.shape[-1])

    place_up(0)
    ln_hop(1)


    period = 2 * UNITS
    lands, shares, works = ([[] for _ in range(period)] for _ in range(3))
    for h in range(1, half + 1):
        for u in range(UNITS):
            landing = 2 * u + h
            work = 2 * u + half + (h > half // 2)
            for table, n in ((lands, landing), (shares, landing + 1), (works, work)):
                table[n % period].append((u, h, n // period))

    def run(action, table, l):
        for late in (0, 1):
            items = [(u, h) for u, h, lateness in table if lateness == late]
            if items:

                @pl.when(l < layers if late == 0 else l > 0)
                def _():
                    for u, h in items:
                        action(l - late, u, h)

    def land(l, u, h):
        forward(l, u, h, 0)
        forward(l, u, h, 1)

    def work(l, u, h):
        compute(l, u, h)
        if u == 0 and h == half:
            for copy in cache_copies(l):
                copy.start()

    def cache_copies(l):
        return [
            pltpu.make_async_copy(src.at[l], dst.at[l], cache_sem.at[l, i])
            for i, (src, dst) in enumerate(((k_ref, k_hbm), (v_ref, v_hbm)))
        ]

    @pl.loop(0, layers + 1)
    def _(l):
        for n in range(period):
            if n % 2 == 0:
                u = n // 2

                @pl.when((l < layers) & (l + u > 0))
                def _():
                    for s in (0, 1):
                        send_own(l, u, s)
                    send_own_sib(l, u)

            run(land, lands[n], l)
            if n in (1, 2, 3):

                @pl.when(l == 0)
                def _():
                    ln_hop(n + 1)
                    if n == 2:
                        for load in loads[1:]:
                            load.wait()
                        for later in range(1, layers):
                            place_up(later)
                    if n == 3:
                        ln_share(c).start()

            run(share_with_sibling, shares[n], l)
            run(work, works[n], l)

    y_t = x_t[...].reshape(-1, x_t.shape[-1])
    for b in range(x_hbm.shape[0]):
        x_nat[b] = y_t[:, b * seq : (b + 1) * seq].T
    store_y = pltpu.make_async_copy(x_nat, y_hbm, load_sem.at[2 * layers + 2])
    store_y.start()

    ref = ln_all.at[c]
    for direction in (0, 1):
        src = ref.at[pl.ds(0, half - direction)]
        remote(src, src, ln_send.at[direction], ln_sib.at[1], dev_z[direction]).wait_send()
    ln_share(c).wait_send()

    @pl.loop(0, layers)
    def _(l):
        for u in range(UNITS):
            sent = bufs[u].at[l, pl.ds(0, chips - 1)]
            for i in (0, 1):
                remote(sent, sent, z_send.at[l * UNITS + u, i], ln_sib.at[1], dev_z[i]).wait_send()
                remote(sent, sent, xy_send.at[l * UNITS + u, i], ln_sib.at[1], dev_xy[i]).wait_send()
            sent = bufs[u].at[l, pl.ds(0, chips * QUARTERS)]
            remote(sent, sent, sib_send.at[l * UNITS + u], ln_sib.at[1], dev_sib).wait_send()
        for copy in cache_copies(l):
            copy.wait()

    store_y.wait()


def solution(mesh):
    batch_spec = P(("dp", "wg"))
    col_spec = P(None, None, "wg")
    out_spec = P(None, None, None, "wg")
    cache_spec = P(None, ("dp", "wg"))
    cols = math.isqrt(mesh.shape["dp"])
    chips = mesh.shape["wg"] // 2

    def local_program(x, positions, prompt_len, ln_attn, ln_mlp, w_qkv, w_out, w_up, w_down):
        prompts, seq, width = x.shape
        layers = w_qkv.shape[0]
        heads, head_dim = w_out.shape[1], w_out.shape[2]
        tokens = prompts * seq
        qkv_t = jnp.swapaxes(w_qkv, 1, 2).reshape(layers, QUARTERS, -1, width)
        down_t = jnp.swapaxes(w_down, 1, 2).reshape(layers, QUARTERS, -1, w_down.shape[1])
        out_nat = w_out.reshape(layers, heads * head_dim, -1)
        up_rows = w_up.shape[2] // QUARTERS
        out_rows = out_nat.shape[2] // QUARTERS
        slots = chips * 2 * QUARTERS
        any_spec = pl.BlockSpec(memory_space=pl.ANY)
        cache = jax.ShapeDtypeStruct((layers, prompts, heads, head_dim, seq), BF16)
        dma = pltpu.SemaphoreType.DMA
        shares = chips * 2
        y, k_cache, v_cache = pl.pallas_call(
            functools.partial(kernel, cols, chips, layers),
            out_shape=(jax.ShapeDtypeStruct(x.shape, BF16), cache, cache),
            in_specs=[pl.BlockSpec(memory_space=pltpu.SMEM)] * 2 + [any_spec] * 7,
            out_specs=(any_spec,) * 3,
            scratch_shapes=[
                pltpu.VMEM((layers, slots) + qkv_t.shape[2:], BF16),
                pltpu.VMEM((layers, slots, up_rows + out_rows, width), BF16),
                pltpu.VMEM((layers, slots) + down_t.shape[2:], BF16),
                pltpu.VMEM(w_up.shape, BF16),
                pltpu.VMEM(out_nat.shape, BF16),
                pltpu.VMEM(x.shape, BF16),
                pltpu.VMEM((shares, width // shares, tokens), BF16),
                pltpu.VMEM((width, tokens), BF16),
                pltpu.VMEM((width, tokens), BF16),
                pltpu.VMEM((heads, head_dim, tokens), BF16),
                pltpu.VMEM((shares, w_up.shape[2], tokens), BF16),
                pltpu.VMEM((shares, width // shares, tokens), F32),
                pltpu.VMEM((2, chips, layers, 8, 128), F32),
                pltpu.VMEM((layers, 8, 128), F32),
                pltpu.VMEM((2,) + ln_attn.shape, BF16),
                pltpu.VMEM((head_dim // 2, seq), F32),
                pltpu.VMEM((head_dim // 2, seq), F32),
                pltpu.VMEM(cache.shape, BF16),
                pltpu.VMEM(cache.shape, BF16),
                dma((layers * UNITS, 4, chips // 2)),
                dma((layers * UNITS, 2, chips - 1)),
                dma((layers * UNITS, chips)),
                dma((layers * UNITS, 2)),
                dma((layers * UNITS, 2)),
                dma((layers * UNITS,)),
                dma((2, chips // 2)),
                dma((2,)),
                dma((2,)),
                dma((2 * layers + 5,)),
                dma((layers, 2)),
            ],
            compiler_params=pltpu.CompilerParams(
                collective_id=0, has_side_effects=True, vmem_limit_bytes=67043328
            ),
        )(positions, prompt_len, x, ln_attn, ln_mlp, qkv_t, w_up, out_nat, down_t)
        order = (0, 1, 4, 2, 3)
        return y, k_cache.transpose(order), v_cache.transpose(order)

    return jax.shard_map(
        local_program,
        mesh=mesh,
        in_specs=(batch_spec, P("dp"), batch_spec, col_spec, col_spec, col_spec, out_spec, col_spec, col_spec),
        out_specs=(batch_spec, cache_spec, cache_spec),
        check_vma=False,
    )
```

```python
import functools
import math

import jax
import jax.numpy as jnp
from jax import lax
from jax.experimental import pallas as pl
from jax.experimental.pallas import tpu as pltpu
from jax.sharding import PartitionSpec as P

EPSILON = 1e-5
ROPE_BASE = 10000.0
MESH = pl.DeviceIdType.MESH
F32 = jnp.float32
BF16 = jnp.bfloat16
QUARTERS = 4
HALF_UP, HALF_DOWN, QKV_0, QKV_1, UP, DOWN = range(6)
UNITS = 6
X_LINK, Y_LINK = 0, 1


def kernel(
    cols,
    chips,
    pos_ref,
    len_ref,
    x_hbm,
    lna_hbm,
    lnm_hbm,
    qkv_hbm,
    up_hbm,
    out_hbm,
    down_hbm,
    y_hbm,
    k_hbm,
    v_hbm,
    buf_hu,
    buf_hd,
    buf_q0,
    buf_q1,
    buf_u,
    buf_d,
    up_half,
    up_nat,
    out_nat,
    x_nat,
    x_other,
    x_t,
    x_other_t,
    a_t,
    m_t,
    ctx_t,
    hid_half,
    hid_t,
    acc,
    part_out,
    part_in,
    ln_all,
    ln_own,
    ln_nat,
    cos_ref,
    sin_ref,
    k_ref,
    v_ref,
    z_recv,
    xy_recv,
    sib_recv,
    part_recv,
    z_send,
    xy_send,
    sib_send,
    part_send,
    ln_recv,
    ln_send,
    ln_sib,
    x_sem,
    load_sem,
    cache_sem,
):
    half = chips // 2
    shares = 2 * chips
    tokens = x_t.shape[-1]
    seq = k_ref.shape[4]
    prompts = k_ref.shape[1]
    layers = k_ref.shape[0]
    d_me = lax.axis_index("dp")
    w_me = lax.axis_index("wg")
    z, c = w_me // 2, w_me % 2
    px, py = (d_me // cols) % 2, (d_me % cols) % 2
    dev_z = ({"wg": lax.rem(z + 1, chips) * 2 + c}, {"wg": lax.rem(z + chips - 1, chips) * 2 + c})
    dev_xy = ({"dp": d_me + cols * (1 - 2 * px)}, {"dp": d_me + 1 - 2 * py})
    dev_sib = {"wg": z * 2 + 1 - c}
    bufs = (buf_hu, buf_hd, buf_q0, buf_q1, buf_u, buf_d)
    hops = ((half, half - 1), (half - 1, half))

    by_quarter = (((px, 1), X_LINK, (1 - px, 1)), ((2 + py, 1), Y_LINK, (3 - py, 1)))
    plans = (
        (((0, 1), None, None), ((1 + px, 1), X_LINK, (2 - px, 1))),
        (((0, 2), None, None), ((2 + px, 1), X_LINK, (3 - px, 1))),
    ) + (by_quarter,) * 4

    def chip_at(direction, h):
        return lax.rem(z + chips - h, chips) if direction == 0 else lax.rem(z + h, chips)

    def pieces(u, chip, which):
        return bufs[u].at[chip * 2 + c, pl.ds(which[0], which[1])]

    def remote(src, dst, send, recv, dev):
        return pltpu.make_async_remote_copy(
            src_ref=src, dst_ref=dst, send_sem=send, recv_sem=recv, device_id=dev, device_id_type=MESH
        )

    def z_link(u, direction, s, h, chip):
        ref = pieces(u, chip, plans[u][s][0])
        return remote(ref, ref, z_send.at[u, direction], z_recv.at[u, direction * 2 + s, h - 1], dev_z[direction])

    def z_copy(u, direction, s, h):
        return z_link(u, direction, s, h, chip_at(direction, h - 1))

    def z_arrival(u, direction, s, h):
        return z_link(u, direction, s, h, chip_at(direction, h))

    def source_index(direction, h):
        return (h - 1) * 2 + direction if h < half else chips - 2

    def xy_copy(u, direction, s, h, which):
        ref = pieces(u, chip_at(direction, h), which)
        link = plans[u][s][1]
        return remote(ref, ref, xy_send.at[u, s], xy_recv.at[u, s, source_index(direction, h)], dev_xy[link])

    def sib_copy(u, chip, core, index):
        ref = bufs[u].at[chip * 2 + core]
        return remote(ref, ref, sib_send.at[u], sib_recv.at[u, index], dev_sib)

    def send_own(u):
        for s in (0, 1):
            for direction in (0, 1):
                z_copy(u, direction, s, 1).start()
        sib_copy(u, z, c, chips - 1).start()

    def land(u, h):
        for s in (0, 1):
            for direction in (0, 1):
                if h > hops[direction][s]:
                    continue
                z_arrival(u, direction, s, h).wait_recv()
                if h < hops[direction][s]:
                    z_copy(u, direction, s, h + 1).start()
                if plans[u][s][1] is not None:
                    xy_copy(u, direction, s, h, plans[u][s][0]).start()

    def sources(h):
        return (0, 1) if h < half else (0,)

    def share_with_sibling(u, h):
        for direction in sources(h):
            for s in (0, 1):
                if plans[u][s][1] is not None:
                    xy_copy(u, direction, s, h, plans[u][s][2]).wait_recv()
            sib_copy(u, chip_at(direction, h), c, source_index(direction, h)).start()

    def wait_sibling(u, h):
        for direction in sources(h):
            sib_copy(u, chip_at(direction, h), 1 - c, source_index(direction, h)).wait_recv()
        if h == half:
            sib_copy(u, z, 1 - c, chips - 1).wait_recv()

    def chip_pair(h, i):
        return lax.rem(z + (chips - h + i * 2 * h if h < half else half + i * half), chips)

    def ln_hop(h):
        for direction in (0, 1):
            limit = half - direction
            if h > limit:
                continue
            ref = ln_all.at[c, chip_at(direction, h)]
            if h > 0:
                remote(ref, ref, ln_send.at[direction], ln_recv.at[direction, h - 1], dev_z[direction]).wait_recv()
            if h < limit:
                src = ln_own if h == 0 else ref
                remote(src, ref, ln_send.at[direction], ln_recv.at[direction, h], dev_z[direction]).start()

    def ln_share(core):
        return remote(ln_all.at[core], ln_all.at[core], ln_sib.at[0], ln_sib.at[1], dev_sib)

    def send_x():
        return remote(x_nat, x_other, x_sem.at[0], x_sem.at[1], dev_xy[Y_LINK])

    def part_copy(chip):
        return remote(part_out.at[chip], part_in.at[chip], part_send.at[0], part_recv.at[chip], dev_xy[Y_LINK])


    def transpose_tokens(dst, src):
        for b in range(prompts):
            dst[:, :, b * seq : (b + 1) * seq] = src[b].T.reshape(dst.shape[0], dst.shape[1], seq)

    def normalize(l, src, first, a_dst):
        rows = src[...].reshape(-1, tokens).astype(F32)
        centered = rows - jnp.mean(rows, axis=0, keepdims=True)
        var = jnp.mean(centered * centered, axis=0, keepdims=True)
        normed = centered * lax.rsqrt(var + EPSILON)
        params = ln_all[:, :, l].reshape(-1, 128).T
        step = src.shape[1]
        for w in range(shares):
            block = normed[w * step : (w + 1) * step]
            base = ((w % 2) * chips + w // 2) * 8
            column = [params[:step, base + r : base + r + 1] for r in range(4)]
            if a_dst is not None:
                a_dst[w * step : (w + 1) * step, :] = (block * column[0] + column[1]).astype(BF16)
            m_t[w * step : (w + 1) * step, first : first + tokens] = (block * column[2] + column[3]).astype(BF16)

    def gelu(pre):
        return (0.5 * pre * (1.0 + lax.erf(pre * 0.5**0.5))).astype(BF16)

    def rotate(vec, cos, sin):
        first, second = vec[: cos.shape[0]].astype(F32), vec[cos.shape[0] :].astype(F32)
        return jnp.concatenate([first * cos - second * sin, second * cos + first * sin], axis=0).astype(BF16)

    def compute_qkv(l, buf, chip):
        head_dim = k_ref.shape[3]
        cos, sin = cos_ref[...], sin_ref[...]
        k_index = lax.broadcasted_iota(jnp.int32, (seq, seq), 0)
        q_index = lax.broadcasted_iota(jnp.int32, (seq, seq), 1)
        for core in (0, 1):
            head = chip * 2 + core
            share = buf[head].reshape(-1, buf.shape[-1])
            qkv = jnp.dot(share, a_t[...], preferred_element_type=F32).astype(BF16)
            for b in range(prompts):
                cols_b = slice(b * seq, (b + 1) * seq)
                q_t = rotate(qkv[:head_dim, cols_b], cos, sin)
                k_t = rotate(qkv[head_dim : 2 * head_dim, cols_b], cos, sin)
                v_t = qkv[2 * head_dim :, cols_b]
                k_ref[l, b, head] = k_t
                v_ref[l, b, head] = v_t
                scores = jnp.dot(k_t.T, q_t, preferred_element_type=F32) * head_dim**-0.5
                allowed = (k_index <= q_index) & (k_index < len_ref[b])
                scores = jnp.where(allowed, scores, -1e30)
                top = jnp.max(scores, axis=0, keepdims=True)
                expo = jnp.exp(scores - top)
                prob = (expo * (1.0 / jnp.sum(expo, axis=0, keepdims=True))).astype(BF16)
                ctx_t[head, :, cols_b] = jnp.dot(v_t, prob, preferred_element_type=F32).astype(BF16)

    def compute_half_up(chip):
        both = pl.ds(chip * 2, 2)
        share = buf_hu[both, 1:].reshape(-1, buf_hu.shape[-1])
        for i in (0, 1):
            cols_i = slice(i * tokens, (i + 1) * tokens)
            pre = jnp.dot(share, m_t[:, cols_i], preferred_element_type=F32)
            hid_half[both, :, cols_i] = gelu(pre).reshape(2, -1, tokens)

    def compute_half_down(chip):
        both = pl.ds(chip * 2, 2)
        share = buf_hd[both].reshape(-1, buf_hd.shape[-1])
        hidden = hid_half[...].reshape(-1, 2 * tokens)
        acc[both] = jnp.dot(share, hidden[:, :tokens], preferred_element_type=F32).reshape((2,) + acc.shape[1:])
        part = jnp.dot(share, hidden[:, tokens:], preferred_element_type=F32)
        part_out[chip] = part.reshape(part_out.shape[1:])

    def finish_layer_0():
        @pl.loop(0, chips)
        def _(chip):
            part_copy(chip).wait_recv()
            both = pl.ds(chip * 2, 2)
            share = buf_hu[both, 0].reshape(-1, buf_hu.shape[-1])
            attn_out = jnp.dot(share, ctx_t[...].reshape(-1, tokens), preferred_element_type=F32)
            mlp_out = acc[both] + part_in[chip]
            x_t[both] = (x_t[both].astype(F32) + attn_out.reshape(mlp_out.shape) + mlp_out).astype(BF16)

    def compute_up(chip):
        up_rows = up_hbm.shape[2] // QUARTERS
        for core in (0, 1):
            share = buf_u[chip * 2 + core, :, :up_rows, :].reshape(-1, buf_u.shape[-1])
            hid_t[chip * 2 + core] = gelu(jnp.dot(share, m_t[:, :tokens], preferred_element_type=F32))
        both = pl.ds(chip * 2, 2)
        share = buf_u[both, :, up_rows:, :].reshape(-1, buf_u.shape[-1])
        attn_out = jnp.dot(share, ctx_t[...].reshape(-1, tokens), preferred_element_type=F32)
        acc[both] = attn_out.reshape((2,) + acc.shape[1:])

    def compute_down(chip):
        both = pl.ds(chip * 2, 2)
        share = buf_d[both].reshape(-1, buf_d.shape[-1])
        hidden = hid_t[...].reshape(-1, tokens)
        mlp_out = jnp.dot(share, hidden, preferred_element_type=F32).reshape((2,) + acc.shape[1:])
        x_t[both] = (x_t[both].astype(F32) + acc[both] + mlp_out).astype(BF16)

    computes = (
        compute_half_up,
        compute_half_down,
        functools.partial(compute_qkv, 0, buf_q0),
        functools.partial(compute_qkv, 1, buf_q1),
        compute_up,
        compute_down,
    )

    def cache_copies(l):
        return [
            pltpu.make_async_copy(src.at[l], dst.at[l], cache_sem.at[l, i])
            for i, (src, dst) in enumerate(((k_ref, k_hbm), (v_ref, v_hbm)))
        ]

    def work(u, h):
        wait_sibling(u, h)
        if (u, h) == (HALF_UP, 1):
            ln_share(1 - c).wait_recv()
            normalize(0, x_t, 0, a_t)
            send_x().wait_recv()
            transpose_tokens(x_other_t, x_other)
            normalize(0, x_other_t, tokens, None)
        if (u, h) == (QKV_1, 1):
            finish_layer_0()
            normalize(1, x_t, 0, a_t)

        @pl.loop(0, 2)
        def _(i):
            computes[u](chip_pair(h, i))

        if h == half and u in (QKV_0, QKV_1):
            for copy in cache_copies(u - QKV_0):
                copy.start()

    def ship(h):
        @pl.loop(0, 2)
        def _(i):
            part_copy(chip_pair(h, i)).start()


    own_half = up_half.shape[1]
    loads = [
        pltpu.make_async_copy(up_hbm.at[0, :, pl.ds(py * own_half, own_half)], up_half, load_sem.at[0]),
        pltpu.make_async_copy(out_hbm, out_nat, load_sem.at[1]),
        pltpu.make_async_copy(x_hbm, x_nat, load_sem.at[2]),
        pltpu.make_async_copy(lna_hbm, ln_nat.at[0], load_sem.at[3]),
        pltpu.make_async_copy(lnm_hbm, ln_nat.at[1], load_sem.at[4]),
        pltpu.make_async_copy(up_hbm.at[1], up_nat, load_sem.at[5]),
        pltpu.make_async_copy(qkv_hbm.at[0], buf_q0.at[w_me], load_sem.at[6]),
        pltpu.make_async_copy(qkv_hbm.at[1], buf_q1.at[w_me], load_sem.at[7]),
        pltpu.make_async_copy(down_hbm.at[1], buf_d.at[w_me], load_sem.at[8]),
    ]
    for load in loads[:5]:
        load.start()
    for w in range(shares):
        pltpu.make_async_copy(
            down_hbm.at[0, :, :, pl.ds(w * 2 * own_half + py * own_half, own_half)],
            buf_hd.at[w_me, :, :, pl.ds(w * own_half, own_half)],
            load_sem.at[9],
        ).start()
    for load in loads[5:]:
        load.start()

    barrier = pltpu.get_barrier_semaphore()
    neighbours = dev_z + dev_xy + (dev_sib,)
    for dev in neighbours:
        pl.semaphore_signal(barrier, inc=1, device_id=dev, device_id_type=MESH)
    loads[0].wait()
    loads[1].wait()
    buf_hu[w_me, 0] = out_nat[0].T
    buf_hu[w_me, 1:] = up_half[...].T.reshape(buf_hu.shape[1] - 1, buf_hu.shape[2], buf_hu.shape[3])
    ln_own[...] = jnp.zeros_like(ln_own)
    for i in (0, 1):
        loads[3 + i].wait()
        for l in range(layers):
            ln_own[l, 2 * i : 2 * i + 2, : ln_nat.shape[3]] = ln_nat[i, l].astype(F32)
    ln_all[c, z] = ln_own[...]
    loads[2].wait()
    pl.semaphore_wait(barrier, len(neighbours))

    send_x().start()
    send_own(0)
    ln_hop(0)
    transpose_tokens(x_t, x_nat)
    half_dim = cos_ref.shape[0]
    row = lax.broadcasted_iota(jnp.int32, cos_ref.shape, 0).astype(F32)
    position = (pos_ref[0] + lax.broadcasted_iota(jnp.int32, cos_ref.shape, 1)).astype(F32)
    angles = position * ROPE_BASE ** (-row * 2.0 / (2 * half_dim))
    cos_ref[...] = jnp.cos(angles)
    sin_ref[...] = jnp.sin(angles)
    ln_hop(1)
    for load in loads[5:]:
        load.wait()
    pltpu.make_async_copy(buf_hd.at[w_me], buf_hd.at[w_me], load_sem.at[9]).wait()
    up_rows = up_hbm.shape[2] // QUARTERS


    lands, gives, works = ([[] for _ in range(2 * UNITS + half)] for _ in range(3))
    for h in range(1, half + 1):
        for u in range(UNITS):
            lands[2 * u + h].append((u, h))
            gives[2 * u + h + 1].append((u, h))
            works[2 * u + half + (h > half // 2)].append((u, h))

    unshipped = []
    for n in range(2 * UNITS + half):
        if n % 2 == 0 and 0 < n < 2 * UNITS:
            send_own(n // 2)
        for u, h in lands[n]:
            land(u, h)
        if n in (1, 2, 3):
            ln_hop(n + 1)
        if n == 2:
            buf_u[w_me, :, :up_rows, :] = up_nat[...].T.reshape(QUARTERS, up_rows, -1)
            buf_u[w_me, :, up_rows:, :] = out_nat[1].T.reshape(QUARTERS, -1, buf_u.shape[-1])
        if n == 3:
            ln_share(c).start()
        for u, h in gives[n]:
            share_with_sibling(u, h)
        for h in unshipped:
            ship(h)
        unshipped = []
        for u, h in works[n]:
            work(u, h)
            for earlier in unshipped:
                ship(earlier)
            unshipped = [h] if u == HALF_DOWN else []

    send_x().wait_send()
    y_t = x_t[...].reshape(-1, tokens)
    for b in range(prompts):
        x_nat[b] = y_t[:, b * seq : (b + 1) * seq].T
    store_y = pltpu.make_async_copy(x_nat, y_hbm, load_sem.at[2])
    store_y.start()

    for direction in (0, 1):
        src = ln_all.at[c, pl.ds(0, half - direction)]
        remote(src, src, ln_send.at[direction], ln_sib.at[1], dev_z[direction]).wait_send()
    ln_share(c).wait_send()
    remote(part_out, part_in, part_send.at[0], ln_sib.at[1], dev_xy[Y_LINK]).wait_send()
    for u in range(UNITS):
        for direction in (0, 1):
            count = sum(hops[direction][s] * plans[u][s][0][1] for s in (0, 1))
            sent = bufs[u].at[pl.ds(0, count), 0]
            remote(sent, sent, z_send.at[u, direction], ln_sib.at[1], dev_z[direction]).wait_send()
        for s in (0, 1):
            if plans[u][s][1] is not None:
                sent = bufs[u].at[pl.ds(0, chips - 1), 0]
                remote(sent, sent, xy_send.at[u, s], ln_sib.at[1], dev_xy[plans[u][s][1]]).wait_send()
        sent = bufs[u].at[pl.ds(0, chips)]
        remote(sent, sent, sib_send.at[u], ln_sib.at[1], dev_sib).wait_send()
    for l in range(layers):
        for copy in cache_copies(l):
            copy.wait()
    store_y.wait()


def solution(mesh):
    batch_spec = P(("dp", "wg"))
    col_spec = P(None, None, "wg")
    out_spec = P(None, None, None, "wg")
    cache_spec = P(None, ("dp", "wg"))
    cols = math.isqrt(mesh.shape["dp"])
    chips = mesh.shape["wg"] // 2

    def local_program(x, positions, prompt_len, ln_attn, ln_mlp, w_qkv, w_out, w_up, w_down):
        prompts, seq, width = x.shape
        layers = w_qkv.shape[0]
        heads, head_dim = w_out.shape[1], w_out.shape[2]
        tokens = prompts * seq
        qkv_t = jnp.swapaxes(w_qkv, 1, 2).reshape(layers, QUARTERS, -1, width)
        down_t = jnp.swapaxes(w_down, 1, 2).reshape(layers, QUARTERS, -1, w_down.shape[1])
        out_nat = w_out.reshape(layers, heads * head_dim, -1)
        up_rows = w_up.shape[2] // QUARTERS
        out_rows = out_nat.shape[2] // QUARTERS
        half_up = w_up.shape[2] // 2
        any_spec = pl.BlockSpec(memory_space=pl.ANY)
        cache = jax.ShapeDtypeStruct((layers, prompts, heads, head_dim, seq), BF16)
        dma = pltpu.SemaphoreType.DMA
        shares = chips * 2
        y, k_cache, v_cache = pl.pallas_call(
            functools.partial(kernel, cols, chips),
            out_shape=(jax.ShapeDtypeStruct(x.shape, BF16), cache, cache),
            in_specs=[pl.BlockSpec(memory_space=pltpu.SMEM)] * 2 + [any_spec] * 7,
            out_specs=(any_spec,) * 3,
            scratch_shapes=[
                pltpu.VMEM((shares, 3, half_up // 2, width), BF16),
                pltpu.VMEM((shares, QUARTERS, down_t.shape[2], down_t.shape[3] // 2), BF16),
                pltpu.VMEM((shares,) + qkv_t.shape[1:], BF16),
                pltpu.VMEM((shares,) + qkv_t.shape[1:], BF16),
                pltpu.VMEM((shares, QUARTERS, up_rows + out_rows, width), BF16),
                pltpu.VMEM((shares,) + down_t.shape[1:], BF16),
                pltpu.VMEM((width, half_up), BF16),
                pltpu.VMEM(w_up.shape[1:], BF16),
                pltpu.VMEM(out_nat.shape, BF16),
                pltpu.VMEM(x.shape, BF16),
                pltpu.VMEM(x.shape, BF16),
                pltpu.VMEM((shares, width // shares, tokens), BF16),
                pltpu.VMEM((shares, width // shares, tokens), BF16),
                pltpu.VMEM((width, tokens), BF16),
                pltpu.VMEM((width, 2 * tokens), BF16),
                pltpu.VMEM((heads, head_dim, tokens), BF16),
                pltpu.VMEM((shares, half_up, 2 * tokens), BF16),
                pltpu.VMEM((shares, w_up.shape[2], tokens), BF16),
                pltpu.VMEM((shares, width // shares, tokens), F32),
                pltpu.VMEM((chips, 2, width // shares, tokens), F32),
                pltpu.VMEM((chips, 2, width // shares, tokens), F32),
                pltpu.VMEM((2, chips, layers, 8, 128), F32),
                pltpu.VMEM((layers, 8, 128), F32),
                pltpu.VMEM((2,) + ln_attn.shape, BF16),
                pltpu.VMEM((head_dim // 2, seq), F32),
                pltpu.VMEM((head_dim // 2, seq), F32),
                pltpu.VMEM(cache.shape, BF16),
                pltpu.VMEM(cache.shape, BF16),
                dma((UNITS, 4, chips // 2)),
                dma((UNITS, 2, chips - 1)),
                dma((UNITS, chips)),
                dma((chips,)),
                dma((UNITS, 2)),
                dma((UNITS, 2)),
                dma((UNITS,)),
                dma((1,)),
                dma((2, chips // 2)),
                dma((2,)),
                dma((2,)),
                dma((2,)),
                dma((10,)),
                dma((layers, 2)),
            ],
            compiler_params=pltpu.CompilerParams(
                collective_id=0, has_side_effects=True, vmem_limit_bytes=67043328
            ),
        )(positions, prompt_len, x, ln_attn, ln_mlp, qkv_t, w_up, out_nat, down_t)
        order = (0, 1, 4, 2, 3)
        return y, k_cache.transpose(order), v_cache.transpose(order)

    return jax.shard_map(
        local_program,
        mesh=mesh,
        in_specs=(batch_spec, P("dp"), batch_spec, col_spec, col_spec, col_spec, out_spec, col_spec, col_spec),
        out_specs=(batch_spec, cache_spec, cache_spec),
        check_vma=False,
    )
```

```python
import functools
import heapq
import math

import jax
import jax.numpy as jnp
from jax import lax
from jax.experimental import pallas as pl
from jax.experimental.pallas import tpu as pltpu
from jax.sharding import PartitionSpec as P

EPSILON = 1e-5
ROPE_BASE = 10000.0
MESH = pl.DeviceIdType.MESH
F32 = jnp.float32
BF16 = jnp.bfloat16
QUARTERS = 4
MODEL = (46.6e3, 300e3, 3.0, 1.5, 2.0, 6.0, 3.0, 0.05)
WORK_US = (1.9, 0.5, 0.7, 0.5, 0.5)
UNITS = 5


def kernel(
    cols,
    chips,
    layers,
    pos_ref,
    len_ref,
    x_hbm,
    lna_hbm,
    lnm_hbm,
    qkv_hbm,
    up_hbm,
    out_hbm,
    down_hbm,
    y_hbm,
    k_hbm,
    v_hbm,
    buf_q,
    buf_u0,
    buf_u1,
    buf_d0,
    buf_d1,
    up_nat,
    out_nat,
    x_nat,
    x_t,
    a_t,
    m_t,
    ctx_t,
    hid_t,
    acc,
    mlp,
    y_nat,
    ln_all,
    ln_own,
    ln_nat,
    cos_ref,
    sin_ref,
    k_ref,
    v_ref,
    z_recv,
    xy_recv,
    sib_recv,
    z_send,
    xy_send,
    sib_send,
    ln_recv,
    ln_send,
    ln_sib,
    load_sem,
    cache_sem,
    y_sem,
):
    half = chips // 2
    seq = x_hbm.shape[1]
    d_me = lax.axis_index("dp")
    w_me = lax.axis_index("wg")
    z, c = w_me // 2, w_me % 2
    x_pos, y_pos = d_me // cols, d_me % cols
    px, py = x_pos % 2, y_pos % 2
    dev_z = ({"wg": lax.rem(z + 1, chips) * 2 + c}, {"wg": lax.rem(z + chips - 1, chips) * 2 + c})
    dev_xy = ({"dp": d_me + cols * (1 - 2 * px)}, {"dp": d_me + 1 - 2 * py})
    dev_sib = {"wg": z * 2 + 1 - c}
    quarter_z = (px, 2 + py)
    quarter_xy = (1 - px, 3 - py)
    bufs = (buf_q, buf_u0, buf_u1, buf_d0, buf_d1)
    hops = ((half, half - 1), (half - 1, half))

    def chip_at(direction, h):
        return lax.rem(z + chips - h, chips) if direction == 0 else lax.rem(z + h, chips)

    def slot(chip, core, quarter):
        return (chip * 2 + core) * QUARTERS + quarter

    def remote(src, dst, send, recv, dev):
        return pltpu.make_async_remote_copy(
            src_ref=src, dst_ref=dst, send_sem=send, recv_sem=recv, device_id=dev, device_id_type=MESH
        )

    def z_copy(l, u, direction, s, h):
        ref = bufs[u].at[l, slot(chip_at(direction, h - 1), c, quarter_z[s])]
        return remote(ref, ref, z_send.at[l * UNITS + u, direction], z_recv.at[l * UNITS + u, direction * 2 + s, h - 1], dev_z[direction])

    def z_arrival(l, u, direction, s, h):
        ref = bufs[u].at[l, slot(chip_at(direction, h), c, quarter_z[s])]
        return remote(ref, ref, z_send.at[l * UNITS + u, direction], z_recv.at[l * UNITS + u, direction * 2 + s, h - 1], dev_z[direction])

    def source_index(direction, h):
        return (h - 1) * 2 + direction if h < half else chips - 2

    def xy_copy(l, u, direction, s, h, quarter):
        ref = bufs[u].at[l, slot(chip_at(direction, h), c, quarter)]
        return remote(ref, ref, xy_send.at[l * UNITS + u, s], xy_recv.at[l * UNITS + u, s, source_index(direction, h)], dev_xy[s])

    def sib_copy(l, u, chip, core, index):
        ref = bufs[u].at[l, pl.ds(slot(chip, core, 0), QUARTERS)]
        return remote(ref, ref, sib_send.at[l * UNITS + u], sib_recv.at[l * UNITS + u, index], dev_sib)

    def send_own(l, u, s):
        for direction in (0, 1):
            z_copy(l, u, direction, s, 1).start()

    def send_own_sib(l, u):
        sib_copy(l, u, z, c, chips - 1).start()

    def land(l, u, direction, s, h):
        z_arrival(l, u, direction, s, h).wait_recv()
        if h < hops[direction][s]:
            z_copy(l, u, direction, s, h + 1).start()
        xy_copy(l, u, direction, s, h, quarter_z[s]).start()

    def sources(h):
        return (0, 1) if h < half else (0,)

    def share_with_sibling(l, u, direction, h):
        for s in (0, 1):
            xy_copy(l, u, direction, s, h, quarter_xy[s]).wait_recv()
        sib_copy(l, u, chip_at(direction, h), c, source_index(direction, h)).start()

    def wait_sibling(l, u, h):
        for direction in sources(h):
            sib_copy(l, u, chip_at(direction, h), 1 - c, source_index(direction, h)).wait_recv()
        if h == half:
            sib_copy(l, u, z, 1 - c, chips - 1).wait_recv()

    def ln_hop(h):
        for direction in (0, 1):
            limit = half - direction
            if h > limit:
                continue
            if h > 0:
                ref = ln_all.at[c, chip_at(direction, h)]
                remote(ref, ref, ln_send.at[direction], ln_recv.at[direction, h - 1], dev_z[direction]).wait_recv()
            if h < limit:
                dst = ln_all.at[c, chip_at(direction, h)]
                src = ln_own if h == 0 else dst
                remote(src, dst, ln_send.at[direction], ln_recv.at[direction, h], dev_z[direction]).start()

    def ln_share(core):
        return remote(ln_all.at[core], ln_all.at[core], ln_sib.at[0], ln_sib.at[1], dev_sib)

    def y_copy(chip):
        columns = y_nat.shape[3]
        dst = y_hbm.at[:, :, pl.ds(pl.multiple_of(chip * columns, columns), columns)]
        return pltpu.make_async_copy(y_nat.at[chip], dst, y_sem.at[chip])


    def normalize(l):
        rows = x_t[...].reshape(-1, x_t.shape[-1]).astype(F32)
        centered = rows - jnp.mean(rows, axis=0, keepdims=True)
        var = jnp.mean(centered * centered, axis=0, keepdims=True)
        normed = centered * lax.rsqrt(var + EPSILON)
        params = ln_all[:, :, l].reshape(-1, 128).T
        step = x_t.shape[1]
        for w in range(2 * chips):
            block = normed[w * step : (w + 1) * step]
            base = ((w % 2) * chips + w // 2) * 8
            column = [params[:step, base + r : base + r + 1] for r in range(4)]
            a_t[w * step : (w + 1) * step, :] = (block * column[0] + column[1]).astype(BF16)
            m_t[w * step : (w + 1) * step, :] = (block * column[2] + column[3]).astype(BF16)

    def rotate(vec, cos, sin):
        first, second = vec[: cos.shape[0]].astype(F32), vec[cos.shape[0] :].astype(F32)
        return jnp.concatenate([first * cos - second * sin, second * cos + first * sin], axis=0).astype(BF16)

    def compute_qkv(l, chip):
        head_dim = k_ref.shape[3]
        seq = k_ref.shape[4]
        cos, sin = cos_ref[...], sin_ref[...]
        k_index = lax.broadcasted_iota(jnp.int32, (seq, seq), 0)
        q_index = lax.broadcasted_iota(jnp.int32, (seq, seq), 1)
        chains = [(core, b) for core in (0, 1) for b in range(k_ref.shape[1])]
        qkvs, q_ts, k_ts, all_scores, probs = {}, {}, {}, {}, {}
        for core in (0, 1):
            share = buf_q[l, pl.ds(slot(chip, core, 0), QUARTERS)]
            share = share.reshape(-1, share.shape[-1])
            qkvs[core] = jnp.dot(share, a_t[...], preferred_element_type=F32).astype(BF16)
        for core, b in chains:
            cols_b = slice(b * seq, (b + 1) * seq)
            qkv = qkvs[core]
            q_ts[core, b] = rotate(qkv[:head_dim, cols_b], cos, sin)
            k_ts[core, b] = rotate(qkv[head_dim : 2 * head_dim, cols_b], cos, sin)
            k_ref[l, b, chip * 2 + core] = k_ts[core, b]
            v_ref[l, b, chip * 2 + core] = qkv[2 * head_dim :, cols_b]
        for chain in chains:
            all_scores[chain] = jnp.dot(k_ts[chain].T, q_ts[chain], preferred_element_type=F32)
        for core, b in chains:
            scores = all_scores[core, b] * head_dim**-0.5
            allowed = (k_index <= q_index) & (k_index < len_ref[b])
            scores = jnp.where(allowed, scores, -1e30)
            top = jnp.max(scores, axis=0, keepdims=True)
            expo = jnp.exp(scores - top)
            probs[core, b] = (expo * (1.0 / jnp.sum(expo, axis=0, keepdims=True))).astype(BF16)
        for core, b in chains:
            cols_b = slice(b * seq, (b + 1) * seq)
            v_t = qkvs[core][2 * head_dim :, cols_b]
            ctx_t[chip * 2 + core, :, cols_b] = jnp.dot(v_t, probs[core, b], preferred_element_type=F32).astype(BF16)

    def up_half(i, share, chip):
        rows = hid_t.shape[1] // 2
        pre = jnp.dot(share.reshape(-1, share.shape[-1]), m_t[...], preferred_element_type=F32)
        hidden = (0.5 * pre * (1.0 + lax.erf(pre * 0.5**0.5))).astype(BF16)
        hid_t[pl.ds(chip * 2, 2), i * rows : (i + 1) * rows, :] = hidden.reshape(2, rows, hidden.shape[-1])

    def compute_up_0(l, chip):
        up_half(0, buf_u0[l, pl.ds(slot(chip, 0, 0), 2 * QUARTERS)], chip)

    def compute_up_1(l, chip):
        both = pl.ds(slot(chip, 0, 0), 2 * QUARTERS)
        rows = buf_u0.shape[2]
        up_half(1, buf_u1[l, both, :rows, :], chip)
        share = buf_u1[l, both, rows:, :]
        share = share.reshape(-1, share.shape[-1])
        ctx = ctx_t[...].reshape(-1, ctx_t.shape[-1])
        attn_out = jnp.dot(share, ctx, preferred_element_type=F32)
        acc[pl.ds(chip * 2, 2)] = attn_out.reshape((2,) + acc.shape[1:])

    def down_half(buf, i, l, chip):
        share = buf[l, pl.ds(slot(chip, 0, 0), 2 * QUARTERS)]
        share = share.reshape(-1, share.shape[-1])
        hidden = hid_t[i * chips : (i + 1) * chips].reshape(-1, hid_t.shape[-1])
        return jnp.dot(share, hidden, preferred_element_type=F32).reshape((2,) + acc.shape[1:])

    def compute_down_0(l, chip):
        mlp[pl.ds(chip * 2, 2)] = down_half(buf_d0, 0, l, chip)

    def compute_down_1(l, chip):
        both = pl.ds(chip * 2, 2)
        mlp_out = mlp[both] + down_half(buf_d1, 1, l, chip)
        rows = (x_t[both].astype(F32) + acc[both] + mlp_out).astype(BF16)
        x_t[both] = rows

        if l == layers - 1:
            block = rows.reshape(-1, rows.shape[-1])
            for b in range(x_nat.shape[0]):
                y_nat[chip, b] = block[:, b * seq : (b + 1) * seq].T
            y_copy(chip).start()

    computes = (compute_qkv, compute_up_0, compute_up_1, compute_down_0, compute_down_1)

    def compute(l, u, h):
        wait_sibling(l, u, h)
        if u == 0 and h == 1:

            if l == 0:
                ln_share(1 - c).wait_recv()
            normalize(l)

        @pl.loop(0, 2)
        def _(i):
            shift = chips - h + i * 2 * h if h < half else half + i * half
            computes[u](l, lax.rem(z + shift, chips))


    own = pl.ds(slot(z, c, 0), QUARTERS)
    loads = [pltpu.make_async_copy(qkv_hbm.at[l], buf_q.at[l, own], load_sem.at[l]) for l in range(layers)]
    width = buf_d0.shape[3]
    loads += [
        pltpu.make_async_copy(down_hbm.at[l, :, :, i * width : (i + 1) * width], dst.at[l, own], load_sem.at[(1 + i) * layers + l])
        for i, dst in enumerate((buf_d0, buf_d1))
        for l in range(layers)
    ]
    load_up = pltpu.make_async_copy(up_hbm, up_nat, load_sem.at[3 * layers + 0])
    load_out = pltpu.make_async_copy(out_hbm, out_nat, load_sem.at[3 * layers + 1])
    load_x = pltpu.make_async_copy(x_hbm, x_nat, load_sem.at[3 * layers + 2])
    load_ln = [pltpu.make_async_copy(src, ln_nat.at[i], load_sem.at[3 * layers + 3 + i]) for i, src in enumerate((lna_hbm, lnm_hbm))]
    for load in [loads[0]] + load_ln + [load_x, load_up, load_out] + loads[1:]:
        load.start()

    barrier = pltpu.get_barrier_semaphore()
    neighbours = dev_z + dev_xy + (dev_sib,)
    for dev in neighbours:
        pl.semaphore_signal(barrier, inc=1, device_id=dev, device_id_type=MESH)
    ln_own[...] = jnp.zeros_like(ln_own)
    for i in (0, 1):
        load_ln[i].wait()
        for l in range(layers):
            ln_own[l, 2 * i : 2 * i + 2, : ln_nat.shape[3]] = ln_nat[i, l].astype(F32)
    ln_all[c, z] = ln_own[...]
    loads[0].wait()
    pl.semaphore_wait(barrier, len(neighbours))

    send_own(0, 0, 0)
    send_own(0, 0, 1)
    ln_hop(0)
    send_own_sib(0, 0)
    load_up.wait()
    load_out.wait()
    def place_up(l):
        up_t = up_nat[l].T
        out_t = out_nat[l].T
        rows = up_t.shape[0] // 2
        half_rows = buf_u0.shape[2]
        buf_u0[l, own] = up_t[:rows].reshape(QUARTERS, half_rows, -1)
        buf_u1[l, own, :half_rows, :] = up_t[rows:].reshape(QUARTERS, half_rows, -1)
        buf_u1[l, own, half_rows:, :] = out_t.reshape(QUARTERS, -1, out_t.shape[-1])

    place_up(0)
    load_x.wait()
    for b in range(x_hbm.shape[0]):
        x_t[:, :, b * seq : (b + 1) * seq] = x_nat[b].T.reshape(x_t.shape[0], x_t.shape[1], seq)
    half_dim = cos_ref.shape[0]
    row = lax.broadcasted_iota(jnp.int32, cos_ref.shape, 0).astype(F32)
    position = (pos_ref[0] + lax.broadcasted_iota(jnp.int32, cos_ref.shape, 1)).astype(F32)
    angles = position * ROPE_BASE ** (-row * 2.0 / (2 * half_dim))
    cos_ref[...] = jnp.cos(angles)
    sin_ref[...] = jnp.sin(angles)
    ln_hop(1)


    def work(l, u, h):
        compute(l, u, h)
        if u == 0 and h == half:
            for copy in cache_copies(l):
                copy.start()

    def cache_copies(l):
        return [
            pltpu.make_async_copy(src.at[l], dst.at[l], cache_sem.at[l, i])
            for i, (src, dst) in enumerate(((k_ref, k_hbm), (v_ref, v_hbm)))
        ]

    sizes = [math.prod(ref.shape[2:]) * 2 for ref in bufs] * layers
    plan = travel_plan(sizes, WORK_US * layers, half)
    seen = [0] * (half + 1)
    for action, n, *where in plan:
        l, u = n // UNITS, n % UNITS
        if action == "own":
            if n == 3:
                for load in loads[1:]:
                    load.wait()
                for later in range(1, layers):
                    place_up(later)
            if n > 0:
                send_own(l, u, 0)
                send_own(l, u, 1)
                send_own_sib(l, u)
        elif action == "z":
            land(l, u, *where)
            h = where[-1]
            if n == 0 and h < half:
                seen[h] += 1
                if seen[h] == 4:
                    ln_hop(h + 1)
                    if h + 1 == half:
                        ln_share(c).start()
        elif action == "give":
            share_with_sibling(l, u, *where)
        else:
            work(l, u, *where)

    ref = ln_all.at[c]
    for direction in (0, 1):
        src = ref.at[pl.ds(0, half - direction)]
        remote(src, src, ln_send.at[direction], ln_sib.at[1], dev_z[direction]).wait_send()
    ln_share(c).wait_send()

    @pl.loop(0, layers)
    def _(l):
        for u in range(UNITS):
            sent = bufs[u].at[l, pl.ds(0, chips - 1)]
            for i in (0, 1):
                remote(sent, sent, z_send.at[l * UNITS + u, i], ln_sib.at[1], dev_z[i]).wait_send()
                remote(sent, sent, xy_send.at[l * UNITS + u, i], ln_sib.at[1], dev_xy[i]).wait_send()
            sent = bufs[u].at[l, pl.ds(0, chips * QUARTERS)]
            remote(sent, sent, sib_send.at[l * UNITS + u], ln_sib.at[1], dev_sib).wait_send()
        for copy in cache_copies(l):
            copy.wait()


    @pl.loop(0, chips)
    def _(chip):
        y_copy(chip).wait()


def travel_plan(sizes, work_us, half):
    link_rate, core_rate, hop_us, core_us, slack, depth, start_us, issue_us = MODEL
    hops = ((half, half - 1), (half - 1, half))
    queue = dict.fromkeys((0, 1, "x", "y", "core"), 0.0)
    events, plan, parts, shared = [], [], {}, set()
    now, started = 0.0, 0
    works = [(u, h) for u in range(len(sizes)) for h in range(1, half + 1)]
    ln_left, ln_time = 4, None

    def send(link, size, tag):
        queue[link] = max(now, queue[link]) + size / (core_rate if link == "core" else link_rate)
        late = 0.0 if tag[0] == "z" else slack
        heapq.heappush(events, (queue[link] + (core_us if link == "core" else hop_us) + late, len(events) + len(plan) * 1000, tag))

    def source(direction, h):
        return (direction, h) if h < half else (0, half)

    def ready(u, h):
        needs = [(u,) + source(direction, h) for direction in ((0, 1) if h < half else (0,))]
        needs += [(u, 0, 0)] if h == half else []
        return ln_time is not None and now >= ln_time and all(need in shared for need in needs)

    while True:
        while started < len(sizes) and min(queue[0], queue[1]) - now < depth:
            plan.append(("own", started))
            for s in (0, 1):
                for direction in (0, 1):
                    send(direction, sizes[started], ("z", started, direction, s, 1))
            send("core", 4 * sizes[started], ("core", started, 0, 0))
            started += 1
            if started == 1:
                now += start_us
        can_work = bool(works) and ready(*works[0])
        if events and (events[0][0] <= now or not can_work):
            at, _, tag = heapq.heappop(events)
            now = max(now, at) + issue_us
            if tag[0] == "core":
                shared.add(tag[1:])
                continue
            _, u, direction, s, h = tag
            if tag[0] == "z":
                plan.append(tag)
                if h < hops[direction][s]:
                    send(direction, sizes[u], ("z", u, direction, s, h + 1))
                send("xy"[s], sizes[u], ("xy", u, direction, s, h))
                if u == 0 and h == half - 1:
                    ln_left -= 1
                    ln_time = now + 2 * hop_us if ln_left == 0 else None
            key = (u,) + source(direction, h)
            parts[key] = parts.get(key, 0) + 1
            if parts[key] == 4:
                plan.append(("give",) + key)
                send("core", 4 * sizes[u], ("core",) + key)
        elif works:
            if not can_work:
                now = max(now, ln_time)
                continue
            u, h = works.pop(0)
            plan.append(("work", u, h))
            now += work_us[u]
        else:
            return plan


def settle_kernel(*refs):
    count = (len(refs) - 2) // 3
    arrays, results, held = refs[:count], refs[count : 2 * count], refs[2 * count : 3 * count]
    read_sem, write_sem = refs[3 * count :]
    parts = [(i, p) for p in range(arrays[0].shape[0]) for i in range(count)]

    def read(i, p):
        return pltpu.make_async_copy(arrays[i].at[p], held[i].at[p], read_sem.at[i, p])

    def write(i, p):
        return pltpu.make_async_copy(held[i].at[p], results[i].at[p], write_sem.at[i, p])

    for i, p in parts:
        read(i, p).start()
    for i, p in parts:
        read(i, p).wait()
        write(i, p).start()
    for i, p in parts:
        write(i, p).wait()


def settle(*arrays):
    any_spec = pl.BlockSpec(memory_space=pl.ANY)
    sem = pltpu.SemaphoreType.DMA((len(arrays), arrays[0].shape[0]))
    return pl.pallas_call(
        settle_kernel,
        out_shape=tuple(jax.ShapeDtypeStruct(a.shape, a.dtype) for a in arrays),
        in_specs=[any_spec] * len(arrays),
        out_specs=(any_spec,) * len(arrays),
        scratch_shapes=[pltpu.VMEM(a.shape, a.dtype) for a in arrays] + [sem, sem],
    )(*arrays)


def solution(mesh):
    batch_spec = P(("dp", "wg"))
    col_spec = P(None, None, "wg")
    out_spec = P(None, None, None, "wg")
    cache_spec = P(None, ("dp", "wg"))
    cols = math.isqrt(mesh.shape["dp"])
    chips = mesh.shape["wg"] // 2

    def local_program(x, positions, prompt_len, ln_attn, ln_mlp, w_qkv, w_out, w_up, w_down):
        prompts, seq, width = x.shape
        layers = w_qkv.shape[0]
        heads, head_dim = w_out.shape[1], w_out.shape[2]
        tokens = prompts * seq
        qkv_t = jnp.swapaxes(w_qkv, 1, 2).reshape(layers, QUARTERS, -1, width)
        down_t = jnp.swapaxes(w_down, 1, 2).reshape(layers, QUARTERS, -1, w_down.shape[1])
        out_nat = w_out.reshape(layers, heads * head_dim, -1)
        up_rows = w_up.shape[2] // QUARTERS
        out_rows = out_nat.shape[2] // QUARTERS
        slots = chips * 2 * QUARTERS
        any_spec = pl.BlockSpec(memory_space=pl.ANY)
        cache = jax.ShapeDtypeStruct((layers, prompts, heads, head_dim, seq), BF16)
        dma = pltpu.SemaphoreType.DMA
        shares = chips * 2
        y, k_cache, v_cache = pl.pallas_call(
            functools.partial(kernel, cols, chips, layers),
            out_shape=(jax.ShapeDtypeStruct(x.shape, BF16), cache, cache),
            in_specs=[pl.BlockSpec(memory_space=pltpu.SMEM)] * 2 + [any_spec] * 7,
            out_specs=(any_spec,) * 3,
            scratch_shapes=[
                pltpu.VMEM((layers, slots) + qkv_t.shape[2:], BF16),
                pltpu.VMEM((layers, slots, up_rows // 2, width), BF16),
                pltpu.VMEM((layers, slots, up_rows // 2 + out_rows, width), BF16),
                pltpu.VMEM((layers, slots, down_t.shape[2], down_t.shape[3] // 2), BF16),
                pltpu.VMEM((layers, slots, down_t.shape[2], down_t.shape[3] // 2), BF16),
                pltpu.VMEM(w_up.shape, BF16),
                pltpu.VMEM(out_nat.shape, BF16),
                pltpu.VMEM(x.shape, BF16),
                pltpu.VMEM((shares, width // shares, tokens), BF16),
                pltpu.VMEM((width, tokens), BF16),
                pltpu.VMEM((width, tokens), BF16),
                pltpu.VMEM((heads, head_dim, tokens), BF16),
                pltpu.VMEM((shares, w_up.shape[2], tokens), BF16),
                pltpu.VMEM((shares, width // shares, tokens), F32),
                pltpu.VMEM((shares, width // shares, tokens), F32),
                pltpu.VMEM((chips, prompts, seq, width // chips), BF16),
                pltpu.VMEM((2, chips, layers, 8, 128), F32),
                pltpu.VMEM((layers, 8, 128), F32),
                pltpu.VMEM((2,) + ln_attn.shape, BF16),
                pltpu.VMEM((head_dim // 2, seq), F32),
                pltpu.VMEM((head_dim // 2, seq), F32),
                pltpu.VMEM(cache.shape, BF16),
                pltpu.VMEM(cache.shape, BF16),
                dma((layers * UNITS, 4, chips // 2)),
                dma((layers * UNITS, 2, chips - 1)),
                dma((layers * UNITS, chips)),
                dma((layers * UNITS, 2)),
                dma((layers * UNITS, 2)),
                dma((layers * UNITS,)),
                dma((2, chips // 2)),
                dma((2,)),
                dma((2,)),
                dma((3 * layers + 5,)),
                dma((layers, 2)),
                dma((chips,)),
            ],
            compiler_params=pltpu.CompilerParams(
                collective_id=0, has_side_effects=True, vmem_limit_bytes=67043328
            ),
        )(positions, prompt_len, x, ln_attn, ln_mlp, qkv_t, w_up, out_nat, down_t)
        y, k_cache, v_cache = settle(y, k_cache, v_cache)
        order = (0, 1, 4, 2, 3)
        return y, k_cache.transpose(order), v_cache.transpose(order)

    return jax.shard_map(
        local_program,
        mesh=mesh,
        in_specs=(batch_spec, P("dp"), batch_spec, col_spec, col_spec, col_spec, out_spec, col_spec, col_spec),
        out_specs=(batch_spec, cache_spec, cache_spec),
        check_vma=False,
    )
```

```python
import functools
import heapq
import math

import jax
import jax.numpy as jnp
from jax import lax
from jax.experimental import pallas as pl
from jax.experimental.pallas import tpu as pltpu
from jax.sharding import PartitionSpec as P

EPSILON = 1e-5
ROPE_BASE = 10000.0
MESH = pl.DeviceIdType.MESH
F32 = jnp.float32
BF16 = jnp.bfloat16
QUARTERS = 4
MODEL = (46.6e3, 300e3, 2.8, 1.5, 2.0, 1.0, 3.5, 0.03)
WORK_US = (1.9, 0.5, 0.7, 0.5, 0.5)
UNITS = 5


def kernel(
    cols,
    chips,
    layers,
    pos_ref,
    len_ref,
    x_hbm,
    lna_hbm,
    lnm_hbm,
    qkv_hbm,
    up_hbm,
    out_hbm,
    down_hbm,
    y_hbm,
    k_hbm,
    v_hbm,
    buf_q,
    buf_u0,
    buf_u1,
    buf_d0,
    buf_d1,
    up_nat,
    out_nat,
    x_nat,
    x_t,
    a_t,
    m_t,
    ctx_t,
    hid_t,
    acc,
    mlp,
    y_nat,
    ln_all,
    ln_own,
    ln_nat,
    cos_ref,
    sin_ref,
    k_ref,
    v_ref,
    z_recv,
    xy_recv,
    sib_recv,
    z_send,
    xy_send,
    sib_send,
    ln_recv,
    ln_send,
    ln_sib,
    load_sem,
    cache_sem,
    y_sem,
):
    half = chips // 2
    seq = x_hbm.shape[1]
    d_me = lax.axis_index("dp")
    w_me = lax.axis_index("wg")
    z, c = w_me // 2, w_me % 2
    x_pos, y_pos = d_me // cols, d_me % cols
    px, py = x_pos % 2, y_pos % 2
    dev_z = ({"wg": lax.rem(z + 1, chips) * 2 + c}, {"wg": lax.rem(z + chips - 1, chips) * 2 + c})
    dev_xy = ({"dp": d_me + cols * (1 - 2 * px)}, {"dp": d_me + 1 - 2 * py})
    dev_sib = {"wg": z * 2 + 1 - c}
    quarter_z = (px, 2 + py)
    quarter_xy = (1 - px, 3 - py)
    bufs = (buf_q, buf_u0, buf_u1, buf_d0, buf_d1)
    hops = ((half, half - 1), (half - 1, half))

    def chip_at(direction, h):
        return lax.rem(z + chips - h, chips) if direction == 0 else lax.rem(z + h, chips)

    def slot(chip, core, quarter):
        return (chip * 2 + core) * QUARTERS + quarter

    def remote(src, dst, send, recv, dev):
        return pltpu.make_async_remote_copy(
            src_ref=src, dst_ref=dst, send_sem=send, recv_sem=recv, device_id=dev, device_id_type=MESH
        )

    def z_copy(l, u, direction, s, h):
        ref = bufs[u].at[l, slot(chip_at(direction, h - 1), c, quarter_z[s])]
        return remote(ref, ref, z_send.at[l * UNITS + u, direction], z_recv.at[l * UNITS + u, direction * 2 + s, h - 1], dev_z[direction])

    def z_arrival(l, u, direction, s, h):
        ref = bufs[u].at[l, slot(chip_at(direction, h), c, quarter_z[s])]
        return remote(ref, ref, z_send.at[l * UNITS + u, direction], z_recv.at[l * UNITS + u, direction * 2 + s, h - 1], dev_z[direction])

    def source_index(direction, h):
        return (h - 1) * 2 + direction if h < half else chips - 2

    def xy_copy(l, u, direction, s, h, quarter):
        ref = bufs[u].at[l, slot(chip_at(direction, h), c, quarter)]
        return remote(ref, ref, xy_send.at[l * UNITS + u, s], xy_recv.at[l * UNITS + u, s, source_index(direction, h)], dev_xy[s])

    def sib_copy(l, u, chip, core, index):
        ref = bufs[u].at[l, pl.ds(slot(chip, core, 0), QUARTERS)]
        return remote(ref, ref, sib_send.at[l * UNITS + u], sib_recv.at[l * UNITS + u, index], dev_sib)

    def send_own(l, u, s):
        for direction in (0, 1):
            z_copy(l, u, direction, s, 1).start()

    def send_own_sib(l, u):
        sib_copy(l, u, z, c, chips - 1).start()

    def land(l, u, direction, s, h):
        z_arrival(l, u, direction, s, h).wait_recv()
        if h < hops[direction][s]:
            z_copy(l, u, direction, s, h + 1).start()
        xy_copy(l, u, direction, s, h, quarter_z[s]).start()

    def sources(h):
        return (0, 1) if h < half else (0,)

    def share_with_sibling(l, u, direction, h):
        for s in (0, 1):
            xy_copy(l, u, direction, s, h, quarter_xy[s]).wait_recv()
        sib_copy(l, u, chip_at(direction, h), c, source_index(direction, h)).start()

    def wait_sibling(l, u, h):
        for direction in sources(h):
            sib_copy(l, u, chip_at(direction, h), 1 - c, source_index(direction, h)).wait_recv()
        if h == half:
            sib_copy(l, u, z, 1 - c, chips - 1).wait_recv()

    def ln_hop(h):
        for direction in (0, 1):
            limit = half - direction
            if h > limit:
                continue
            if h > 0:
                ref = ln_all.at[c, chip_at(direction, h)]
                remote(ref, ref, ln_send.at[direction], ln_recv.at[direction, h - 1], dev_z[direction]).wait_recv()
            if h < limit:
                dst = ln_all.at[c, chip_at(direction, h)]
                src = ln_own if h == 0 else dst
                remote(src, dst, ln_send.at[direction], ln_recv.at[direction, h], dev_z[direction]).start()

    def ln_share(core):
        return remote(ln_all.at[core], ln_all.at[core], ln_sib.at[0], ln_sib.at[1], dev_sib)

    def y_copy(chip):
        columns = y_nat.shape[3]
        dst = y_hbm.at[:, :, pl.ds(pl.multiple_of(chip * columns, columns), columns)]
        return pltpu.make_async_copy(y_nat.at[chip], dst, y_sem.at[chip])


    def normalize(l):
        rows = x_t[...].reshape(-1, x_t.shape[-1]).astype(F32)
        centered = rows - jnp.mean(rows, axis=0, keepdims=True)
        var = jnp.mean(centered * centered, axis=0, keepdims=True)
        normed = centered * lax.rsqrt(var + EPSILON)
        params = ln_all[:, :, l].reshape(-1, 128).T
        step = x_t.shape[1]
        for w in range(2 * chips):
            block = normed[w * step : (w + 1) * step]
            base = ((w % 2) * chips + w // 2) * 8
            column = [params[:step, base + r : base + r + 1] for r in range(4)]
            a_t[w * step : (w + 1) * step, :] = (block * column[0] + column[1]).astype(BF16)
            m_t[w * step : (w + 1) * step, :] = (block * column[2] + column[3]).astype(BF16)

    def rotate(vec, cos, sin):
        first, second = vec[: cos.shape[0]].astype(F32), vec[cos.shape[0] :].astype(F32)
        return jnp.concatenate([first * cos - second * sin, second * cos + first * sin], axis=0).astype(BF16)

    def compute_qkv(l, chip):
        head_dim = k_ref.shape[3]
        seq = k_ref.shape[4]
        cos, sin = cos_ref[...], sin_ref[...]
        k_index = lax.broadcasted_iota(jnp.int32, (seq, seq), 0)
        q_index = lax.broadcasted_iota(jnp.int32, (seq, seq), 1)
        chains = [(core, b) for core in (0, 1) for b in range(k_ref.shape[1])]
        qkvs, q_ts, k_ts, all_scores, probs = {}, {}, {}, {}, {}
        for core in (0, 1):
            share = buf_q[l, pl.ds(slot(chip, core, 0), QUARTERS)]
            share = share.reshape(-1, share.shape[-1])
            qkvs[core] = jnp.dot(share, a_t[...], preferred_element_type=F32).astype(BF16)
        for core, b in chains:
            cols_b = slice(b * seq, (b + 1) * seq)
            qkv = qkvs[core]
            q_ts[core, b] = rotate(qkv[:head_dim, cols_b], cos, sin)
            k_ts[core, b] = rotate(qkv[head_dim : 2 * head_dim, cols_b], cos, sin)
            k_ref[l, b, chip * 2 + core] = k_ts[core, b]
            v_ref[l, b, chip * 2 + core] = qkv[2 * head_dim :, cols_b]
        for chain in chains:
            all_scores[chain] = jnp.dot(k_ts[chain].T, q_ts[chain], preferred_element_type=F32)
        for core, b in chains:
            scores = all_scores[core, b] * head_dim**-0.5
            allowed = (k_index <= q_index) & (k_index < len_ref[b])
            scores = jnp.where(allowed, scores, -1e30)
            top = jnp.max(scores, axis=0, keepdims=True)
            expo = jnp.exp(scores - top)
            probs[core, b] = (expo * (1.0 / jnp.sum(expo, axis=0, keepdims=True))).astype(BF16)
        for core, b in chains:
            cols_b = slice(b * seq, (b + 1) * seq)
            v_t = qkvs[core][2 * head_dim :, cols_b]
            ctx_t[chip * 2 + core, :, cols_b] = jnp.dot(v_t, probs[core, b], preferred_element_type=F32).astype(BF16)

    def up_half(i, share, chip):
        rows = hid_t.shape[1] // 2
        pre = jnp.dot(share.reshape(-1, share.shape[-1]), m_t[...], preferred_element_type=F32)
        hidden = (0.5 * pre * (1.0 + lax.erf(pre * 0.5**0.5))).astype(BF16)
        hid_t[pl.ds(chip * 2, 2), i * rows : (i + 1) * rows, :] = hidden.reshape(2, rows, hidden.shape[-1])

    def compute_up_0(l, chip):
        up_half(0, buf_u0[l, pl.ds(slot(chip, 0, 0), 2 * QUARTERS)], chip)

    def compute_up_1(l, chip):
        both = pl.ds(slot(chip, 0, 0), 2 * QUARTERS)
        rows = buf_u0.shape[2]
        up_half(1, buf_u1[l, both, :rows, :], chip)
        share = buf_u1[l, both, rows:, :]
        share = share.reshape(-1, share.shape[-1])
        ctx = ctx_t[...].reshape(-1, ctx_t.shape[-1])
        attn_out = jnp.dot(share, ctx, preferred_element_type=F32)
        acc[pl.ds(chip * 2, 2)] = attn_out.reshape((2,) + acc.shape[1:])

    def down_half(buf, i, l, chip):
        share = buf[l, pl.ds(slot(chip, 0, 0), 2 * QUARTERS)]
        share = share.reshape(-1, share.shape[-1])
        hidden = hid_t[i * chips : (i + 1) * chips].reshape(-1, hid_t.shape[-1])
        return jnp.dot(share, hidden, preferred_element_type=F32).reshape((2,) + acc.shape[1:])

    def compute_down_0(l, chip):
        mlp[pl.ds(chip * 2, 2)] = down_half(buf_d0, 0, l, chip)

    def compute_down_1(l, chip):
        both = pl.ds(chip * 2, 2)
        mlp_out = mlp[both] + down_half(buf_d1, 1, l, chip)
        rows = (x_t[both].astype(F32) + acc[both] + mlp_out).astype(BF16)
        x_t[both] = rows

        if l == layers - 1:
            block = rows.reshape(-1, rows.shape[-1])
            for b in range(x_nat.shape[0]):
                y_nat[chip, b] = block[:, b * seq : (b + 1) * seq].T
            y_copy(chip).start()

    computes = (compute_qkv, compute_up_0, compute_up_1, compute_down_0, compute_down_1)

    def compute(l, u, h):
        wait_sibling(l, u, h)
        if u == 0 and h == 1:

            if l == 0:
                ln_share(1 - c).wait_recv()
            normalize(l)

        @pl.loop(0, 2)
        def _(i):
            shift = chips - h + i * 2 * h if h < half else half + i * half
            computes[u](l, lax.rem(z + shift, chips))


    own = pl.ds(slot(z, c, 0), QUARTERS)
    loads = [pltpu.make_async_copy(qkv_hbm.at[l], buf_q.at[l, own], load_sem.at[l]) for l in range(layers)]
    width = buf_d0.shape[3]
    loads += [
        pltpu.make_async_copy(down_hbm.at[l, :, :, i * width : (i + 1) * width], dst.at[l, own], load_sem.at[(1 + i) * layers + l])
        for i, dst in enumerate((buf_d0, buf_d1))
        for l in range(layers)
    ]
    load_up = pltpu.make_async_copy(up_hbm, up_nat, load_sem.at[3 * layers + 0])
    load_out = pltpu.make_async_copy(out_hbm, out_nat, load_sem.at[3 * layers + 1])
    load_x = pltpu.make_async_copy(x_hbm, x_nat, load_sem.at[3 * layers + 2])
    load_ln = [pltpu.make_async_copy(src, ln_nat.at[i], load_sem.at[3 * layers + 3 + i]) for i, src in enumerate((lna_hbm, lnm_hbm))]
    for load in [loads[0]] + load_ln + [load_x, load_up, load_out] + loads[1:]:
        load.start()

    barrier = pltpu.get_barrier_semaphore()
    neighbours = dev_z + dev_xy + (dev_sib,)
    for dev in neighbours:
        pl.semaphore_signal(barrier, inc=1, device_id=dev, device_id_type=MESH)
    loads[0].wait()
    pl.semaphore_wait(barrier, len(neighbours))

    send_own(0, 0, 0)
    send_own(0, 0, 1)
    send_own_sib(0, 0)
    ln_own[...] = jnp.zeros_like(ln_own)
    for i in (0, 1):
        load_ln[i].wait()
        for l in range(layers):
            ln_own[l, 2 * i : 2 * i + 2, : ln_nat.shape[3]] = ln_nat[i, l].astype(F32)
    ln_all[c, z] = ln_own[...]
    load_up.wait()
    load_out.wait()
    def place_up(l):
        up_t = up_nat[l].T
        out_t = out_nat[l].T
        rows = up_t.shape[0] // 2
        half_rows = buf_u0.shape[2]
        buf_u0[l, own] = up_t[:rows].reshape(QUARTERS, half_rows, -1)
        buf_u1[l, own, :half_rows, :] = up_t[rows:].reshape(QUARTERS, half_rows, -1)
        buf_u1[l, own, half_rows:, :] = out_t.reshape(QUARTERS, -1, out_t.shape[-1])

    place_up(0)
    ln_hop(0)
    load_x.wait()
    for b in range(x_hbm.shape[0]):
        x_t[:, :, b * seq : (b + 1) * seq] = x_nat[b].T.reshape(x_t.shape[0], x_t.shape[1], seq)
    half_dim = cos_ref.shape[0]
    row = lax.broadcasted_iota(jnp.int32, cos_ref.shape, 0).astype(F32)
    position = (pos_ref[0] + lax.broadcasted_iota(jnp.int32, cos_ref.shape, 1)).astype(F32)
    angles = position * ROPE_BASE ** (-row * 2.0 / (2 * half_dim))
    cos_ref[...] = jnp.cos(angles)
    sin_ref[...] = jnp.sin(angles)
    ln_hop(1)


    def work(l, u, h):
        compute(l, u, h)
        if u == 0 and h == half:
            for copy in cache_copies(l):
                copy.start()

    def cache_copies(l):
        return [
            pltpu.make_async_copy(src.at[l], dst.at[l], cache_sem.at[l, i])
            for i, (src, dst) in enumerate(((k_ref, k_hbm), (v_ref, v_hbm)))
        ]

    sizes = [math.prod(ref.shape[2:]) * 2 for ref in bufs] * layers
    plan = travel_plan(sizes, WORK_US * layers, half)
    seen = [0] * (half + 1)
    for action, n, *where in plan:
        l, u = n // UNITS, n % UNITS
        if action == "own":
            if n == 3:
                for load in loads[1:]:
                    load.wait()
                for later in range(1, layers):
                    place_up(later)
            if n > 0:
                send_own(l, u, 0)
                send_own(l, u, 1)
                send_own_sib(l, u)
        elif action == "z":
            land(l, u, *where)
            h = where[-1]
            if n == 0 and h < half:
                seen[h] += 1
                if seen[h] == 4:
                    ln_hop(h + 1)
                    if h + 1 == half:
                        ln_share(c).start()
        elif action == "give":
            share_with_sibling(l, u, *where)
        else:
            work(l, u, *where)

    ref = ln_all.at[c]
    for direction in (0, 1):
        src = ref.at[pl.ds(0, half - direction)]
        remote(src, src, ln_send.at[direction], ln_sib.at[1], dev_z[direction]).wait_send()
    ln_share(c).wait_send()

    @pl.loop(0, layers)
    def _(l):
        for u in range(UNITS):
            sent = bufs[u].at[l, pl.ds(0, chips - 1)]
            for i in (0, 1):
                remote(sent, sent, z_send.at[l * UNITS + u, i], ln_sib.at[1], dev_z[i]).wait_send()
                remote(sent, sent, xy_send.at[l * UNITS + u, i], ln_sib.at[1], dev_xy[i]).wait_send()
            sent = bufs[u].at[l, pl.ds(0, chips * QUARTERS)]
            remote(sent, sent, sib_send.at[l * UNITS + u], ln_sib.at[1], dev_sib).wait_send()
        for copy in cache_copies(l):
            copy.wait()


    @pl.loop(0, chips)
    def _(chip):
        y_copy(chip).wait()


def travel_plan(sizes, work_us, half):
    link_rate, core_rate, hop_us, core_us, slack, depth, start_us, issue_us = MODEL
    hops = ((half, half - 1), (half - 1, half))
    queue = dict.fromkeys((0, 1, "x", "y", "core"), 0.0)
    events, plan, parts, shared = [], [], {}, set()
    now, started = 0.0, 0
    works = [(u, h) for u in range(len(sizes)) for h in range(1, half + 1)]
    ln_left, ln_time = 4, None

    def send(link, size, tag):
        queue[link] = max(now, queue[link]) + size / (core_rate if link == "core" else link_rate)
        late = 0.0 if tag[0] == "z" else slack
        heapq.heappush(events, (queue[link] + (core_us if link == "core" else hop_us) + late, len(events) + len(plan) * 1000, tag))

    def source(direction, h):
        return (direction, h) if h < half else (0, half)

    def ready(u, h):
        needs = [(u,) + source(direction, h) for direction in ((0, 1) if h < half else (0,))]
        needs += [(u, 0, 0)] if h == half else []
        return ln_time is not None and now >= ln_time and all(need in shared for need in needs)

    while True:
        while started < len(sizes) and min(queue[0], queue[1]) - now < depth:
            plan.append(("own", started))
            for s in (0, 1):
                for direction in (0, 1):
                    send(direction, sizes[started], ("z", started, direction, s, 1))
            send("core", 4 * sizes[started], ("core", started, 0, 0))
            started += 1
            if started == 1:
                now += start_us
        can_work = bool(works) and ready(*works[0])
        if events and (events[0][0] <= now or not can_work):
            at, _, tag = heapq.heappop(events)
            now = max(now, at) + issue_us
            if tag[0] == "core":
                shared.add(tag[1:])
                continue
            _, u, direction, s, h = tag
            if tag[0] == "z":
                plan.append(tag)
                if h < hops[direction][s]:
                    send(direction, sizes[u], ("z", u, direction, s, h + 1))
                send("xy"[s], sizes[u], ("xy", u, direction, s, h))
                if u == 0 and h == half - 1:
                    ln_left -= 1
                    ln_time = now + 2 * hop_us if ln_left == 0 else None
            key = (u,) + source(direction, h)
            parts[key] = parts.get(key, 0) + 1
            if parts[key] == 4:
                plan.append(("give",) + key)
                send("core", 4 * sizes[u], ("core",) + key)
        elif works:
            if not can_work:
                now = max(now, ln_time)
                continue
            u, h = works.pop(0)
            plan.append(("work", u, h))
            now += work_us[u]
        else:
            return plan


def settle_kernel(*refs):
    count = (len(refs) - 2) // 3
    arrays, results, held = refs[:count], refs[count : 2 * count], refs[2 * count : 3 * count]
    read_sem, write_sem = refs[3 * count :]
    parts = [(i, p) for p in range(arrays[0].shape[0]) for i in range(count)]

    def read(i, p):
        return pltpu.make_async_copy(arrays[i].at[p], held[i].at[p], read_sem.at[i, p])

    def write(i, p):
        return pltpu.make_async_copy(held[i].at[p], results[i].at[p], write_sem.at[i, p])

    for i, p in parts:
        read(i, p).start()
    for i, p in parts:
        read(i, p).wait()
        write(i, p).start()
    for i, p in parts:
        write(i, p).wait()


def settle(*arrays):
    any_spec = pl.BlockSpec(memory_space=pl.ANY)
    sem = pltpu.SemaphoreType.DMA((len(arrays), arrays[0].shape[0]))
    return pl.pallas_call(
        settle_kernel,
        out_shape=tuple(jax.ShapeDtypeStruct(a.shape, a.dtype) for a in arrays),
        in_specs=[any_spec] * len(arrays),
        out_specs=(any_spec,) * len(arrays),
        scratch_shapes=[pltpu.VMEM(a.shape, a.dtype) for a in arrays] + [sem, sem],
    )(*arrays)


def solution(mesh):
    batch_spec = P(("dp", "wg"))
    col_spec = P(None, None, "wg")
    out_spec = P(None, None, None, "wg")
    cache_spec = P(None, ("dp", "wg"))
    cols = math.isqrt(mesh.shape["dp"])
    chips = mesh.shape["wg"] // 2

    def local_program(x, positions, prompt_len, ln_attn, ln_mlp, w_qkv, w_out, w_up, w_down):
        prompts, seq, width = x.shape
        layers = w_qkv.shape[0]
        heads, head_dim = w_out.shape[1], w_out.shape[2]
        tokens = prompts * seq
        qkv_t = jnp.swapaxes(w_qkv, 1, 2).reshape(layers, QUARTERS, -1, width)
        down_t = jnp.swapaxes(w_down, 1, 2).reshape(layers, QUARTERS, -1, w_down.shape[1])
        out_nat = w_out.reshape(layers, heads * head_dim, -1)
        up_rows = w_up.shape[2] // QUARTERS
        out_rows = out_nat.shape[2] // QUARTERS
        slots = chips * 2 * QUARTERS
        any_spec = pl.BlockSpec(memory_space=pl.ANY)
        cache = jax.ShapeDtypeStruct((layers, prompts, heads, head_dim, seq), BF16)
        dma = pltpu.SemaphoreType.DMA
        shares = chips * 2
        y, k_cache, v_cache = pl.pallas_call(
            functools.partial(kernel, cols, chips, layers),
            out_shape=(jax.ShapeDtypeStruct(x.shape, BF16), cache, cache),
            in_specs=[pl.BlockSpec(memory_space=pltpu.SMEM)] * 2 + [any_spec] * 7,
            out_specs=(any_spec,) * 3,
            scratch_shapes=[
                pltpu.VMEM((layers, slots) + qkv_t.shape[2:], BF16),
                pltpu.VMEM((layers, slots, up_rows // 2, width), BF16),
                pltpu.VMEM((layers, slots, up_rows // 2 + out_rows, width), BF16),
                pltpu.VMEM((layers, slots, down_t.shape[2], down_t.shape[3] // 2), BF16),
                pltpu.VMEM((layers, slots, down_t.shape[2], down_t.shape[3] // 2), BF16),
                pltpu.VMEM(w_up.shape, BF16),
                pltpu.VMEM(out_nat.shape, BF16),
                pltpu.VMEM(x.shape, BF16),
                pltpu.VMEM((shares, width // shares, tokens), BF16),
                pltpu.VMEM((width, tokens), BF16),
                pltpu.VMEM((width, tokens), BF16),
                pltpu.VMEM((heads, head_dim, tokens), BF16),
                pltpu.VMEM((shares, w_up.shape[2], tokens), BF16),
                pltpu.VMEM((shares, width // shares, tokens), F32),
                pltpu.VMEM((shares, width // shares, tokens), F32),
                pltpu.VMEM((chips, prompts, seq, width // chips), BF16),
                pltpu.VMEM((2, chips, layers, 8, 128), F32),
                pltpu.VMEM((layers, 8, 128), F32),
                pltpu.VMEM((2,) + ln_attn.shape, BF16),
                pltpu.VMEM((head_dim // 2, seq), F32),
                pltpu.VMEM((head_dim // 2, seq), F32),
                pltpu.VMEM(cache.shape, BF16),
                pltpu.VMEM(cache.shape, BF16),
                dma((layers * UNITS, 4, chips // 2)),
                dma((layers * UNITS, 2, chips - 1)),
                dma((layers * UNITS, chips)),
                dma((layers * UNITS, 2)),
                dma((layers * UNITS, 2)),
                dma((layers * UNITS,)),
                dma((2, chips // 2)),
                dma((2,)),
                dma((2,)),
                dma((3 * layers + 5,)),
                dma((layers, 2)),
                dma((chips,)),
            ],
            compiler_params=pltpu.CompilerParams(
                collective_id=0, has_side_effects=True, vmem_limit_bytes=67043328
            ),
        )(positions, prompt_len, x, ln_attn, ln_mlp, qkv_t, w_up, out_nat, down_t)
        y, k_cache, v_cache = settle(y, k_cache, v_cache)
        order = (0, 1, 4, 2, 3)
        return y, k_cache.transpose(order), v_cache.transpose(order)

    return jax.shard_map(
        local_program,
        mesh=mesh,
        in_specs=(batch_spec, P("dp"), batch_spec, col_spec, col_spec, col_spec, out_spec, col_spec, col_spec),
        out_specs=(batch_spec, cache_spec, cache_spec),
        check_vma=False,
    )
```
